32 devices in a mesh: dp: 1 (over z), sp: 32 (over y, x, core).
Axes of the slice: x: 4, y: 4, z: 1, core: 2. Of those that a mesh axis runs over, the one named last changes fastest.
The devices are a block of a 4x4x8 slice.
Arguments:
- x: bfloat16 [16384, 2560], P(('dp', 'sp'))
- doc_start: int32 [16384], P(('dp', 'sp'))
- w_in: bfloat16 [2560, 10576], replicated
- conv_w: float32 [4, 5376], replicated
- conv_b: float32 [5376], replicated
- dt_bias: float32 [80], replicated
- a_log: float32 [80], replicated
- d_skip: float32 [80], replicated
- norm_w: float32 [1, 5120], replicated
- w_out: bfloat16 [5120, 2560], replicated
Outputs:
- output: bfloat16 [16384, 2560], P(('dp', 'sp'))
All inputs are finite; a program needn't handle non-finite values.
Results may differ from the reference program's by a relative error of at most 0.00215957.
Values are sent between devices in bfloat16 or wider.
A program may use at most 768 MiB of HBM per device.

```python
import jax
import jax.numpy as jnp
from jax import lax

SEQ_LEN = 16384
SHARD_LEN = 512
D_MODEL = 2560
NUM_HEADS = 80
HEAD_DIM = 64
NUM_GROUPS = 1
STATE_DIM = 128
CHUNK_LEN = 256
CONV_WIDTH = 4
NORM_EPS = 1e-5
D_INNER = NUM_HEADS * HEAD_DIM
GROUP_WIDTH = D_INNER // NUM_GROUPS
PER_GROUP = NUM_HEADS // NUM_GROUPS
CONV_DIM = D_INNER + 2 * NUM_GROUPS * STATE_DIM
PROJ_DIM = 2 * D_INNER + 2 * NUM_GROUPS * STATE_DIM + NUM_HEADS
N_CHUNKS = SEQ_LEN // CHUNK_LEN
N_SHARDS = SEQ_LEN // SHARD_LEN


def draw_starts(start_key):
    level_key, pos_key = jax.random.split(start_key)
    shard_level = jax.random.randint(level_key, (N_SHARDS, 1), 0, 4)
    pos_draws = jax.random.randint(pos_key, (N_SHARDS, SHARD_LEN), 0, SHARD_LEN)
    return (pos_draws < shard_level).astype(jnp.int32).reshape(SEQ_LEN)


def setup_inputs(seed: int = 0, part: int = 0) -> dict:
    root_key = jax.random.key(seed)
    part_key = jax.random.fold_in(root_key, part)
    x_key, start_key = jax.random.split(part_key)
    weight_keys = jax.random.split(root_key, 8)
    x = jax.random.normal(x_key, (SEQ_LEN, D_MODEL), jnp.float32).astype(jnp.bfloat16)
    doc_start = draw_starts(start_key)
    w_in = (jax.random.normal(weight_keys[0], (D_MODEL, PROJ_DIM), jnp.float32) * D_MODEL ** -0.5).astype(jnp.bfloat16)
    conv_w = jax.random.normal(weight_keys[1], (CONV_WIDTH, CONV_DIM), jnp.float32) * 0.5
    conv_b = jax.random.normal(weight_keys[2], (CONV_DIM,), jnp.float32) * 0.5
    dt_bias = jax.random.uniform(weight_keys[3], (NUM_HEADS,), jnp.float32, -3.5, -2.5)
    decay_rate = jax.random.uniform(weight_keys[4], (NUM_HEADS,), jnp.float32, 0.3, 1.5)
    a_log = jnp.log(decay_rate) - jnp.log(0.08 * SHARD_LEN)
    d_skip = jax.random.uniform(weight_keys[5], (NUM_HEADS,), jnp.float32, 0.5, 1.5)
    norm_w = jax.random.uniform(weight_keys[6], (NUM_GROUPS, GROUP_WIDTH), jnp.float32, 0.5, 1.5)
    w_out = (jax.random.normal(weight_keys[7], (D_INNER, D_MODEL), jnp.float32) * D_INNER ** -0.5).astype(jnp.bfloat16)
    return {'x': x, 'doc_start': doc_start, 'w_in': w_in, 'conv_w': conv_w, 'conv_b': conv_b, 'dt_bias': dt_bias, 'a_log': a_log, 'd_skip': d_skip, 'norm_w': norm_w, 'w_out': w_out}


def chunk_step(run_state, chunk_in):
    xs_blk, b_blk, c_blk, dt_blk, ld_blk, start_blk = chunk_in
    cum_decay = jnp.cumsum(ld_blk, axis=0)
    seg_ids = jnp.cumsum(start_blk)
    position = jnp.arange(CHUNK_LEN)
    allowed = (position[:, None] >= position[None, :]) & (seg_ids[:, None] == seg_ids[None, :])
    cum_rows = jnp.moveaxis(cum_decay, 0, -1)
    decay_mat = jnp.exp(jnp.where(allowed, cum_rows[..., :, None] - cum_rows[..., None, :], -jnp.inf))
    scores = jnp.einsum('ign,jgn->gij', c_blk.astype(jnp.float32), b_blk.astype(jnp.float32))
    mix_mat = (scores[:, None] * decay_mat * jnp.moveaxis(dt_blk, 0, -1)[..., None, :]).astype(jnp.bfloat16)
    y_intra = jnp.einsum('gkij,jgkp->igkp', mix_mat.astype(jnp.float32), xs_blk.astype(jnp.float32))
    w_start = jnp.exp(cum_decay) * (seg_ids == 0)[:, None, None]
    y_state = jnp.einsum('ign,gkpn->igkp', c_blk.astype(jnp.float32), run_state.astype(jnp.bfloat16).astype(jnp.float32)) * w_start[..., None]
    last_cum = cum_decay[-1]
    w_end = jnp.exp(last_cum - cum_decay) * dt_blk * (seg_ids == seg_ids[-1])[:, None, None]
    scaled_x = (xs_blk.astype(jnp.float32) * w_end[..., None]).astype(jnp.bfloat16)
    chunk_state = jnp.einsum('jgkp,jgn->gkpn', scaled_x.astype(jnp.float32), b_blk.astype(jnp.float32))
    next_state = (jnp.exp(last_cum) * (seg_ids[-1] == 0))[..., None, None] * run_state + chunk_state
    return next_state, y_intra + y_state


def reference(x, doc_start, w_in, conv_w, conv_b, dt_bias, a_log, d_skip, norm_w, w_out):
    projected = jnp.dot(x, w_in, preferred_element_type=jnp.float32).astype(jnp.bfloat16)
    gate_in = projected[:, :D_INNER].astype(jnp.float32)
    conv_in = projected[:, D_INNER:D_INNER + CONV_DIM].astype(jnp.float32)
    dt_raw = projected[:, D_INNER + CONV_DIM:].astype(jnp.float32)
    keep_flag = (1 - doc_start).astype(jnp.float32)
    keep_pad = jnp.concatenate([jnp.ones((CONV_WIDTH - 1,), jnp.float32), keep_flag])
    conv_pad = jnp.concatenate([jnp.zeros((CONV_WIDTH - 1, CONV_DIM), jnp.float32), conv_in])
    pre_act = conv_b + conv_w[0] * conv_in
    tap_mask = jnp.ones((SEQ_LEN,), jnp.float32)
    for offset in range(1, CONV_WIDTH):
        tap_mask = tap_mask * keep_pad[CONV_WIDTH - offset:CONV_WIDTH - offset + SEQ_LEN]
        pre_act = pre_act + conv_w[offset] * tap_mask[:, None] * conv_pad[CONV_WIDTH - 1 - offset:CONV_WIDTH - 1 - offset + SEQ_LEN]
    conv_out = jax.nn.silu(pre_act).astype(jnp.bfloat16)
    xs_heads = conv_out[:, :D_INNER]
    b_mat = conv_out[:, D_INNER:D_INNER + NUM_GROUPS * STATE_DIM]
    c_mat = conv_out[:, D_INNER + NUM_GROUPS * STATE_DIM:]
    dt_val = jax.nn.softplus(dt_raw + dt_bias)
    log_decay = -jnp.exp(a_log) * dt_val
    chunk_inputs = (
        xs_heads.reshape(N_CHUNKS, CHUNK_LEN, NUM_GROUPS, PER_GROUP, HEAD_DIM),
        b_mat.reshape(N_CHUNKS, CHUNK_LEN, NUM_GROUPS, STATE_DIM),
        c_mat.reshape(N_CHUNKS, CHUNK_LEN, NUM_GROUPS, STATE_DIM),
        dt_val.reshape(N_CHUNKS, CHUNK_LEN, NUM_GROUPS, PER_GROUP),
        log_decay.reshape(N_CHUNKS, CHUNK_LEN, NUM_GROUPS, PER_GROUP),
        doc_start.reshape(N_CHUNKS, CHUNK_LEN),
    )
    zero_state = jnp.zeros((NUM_GROUPS, PER_GROUP, HEAD_DIM, STATE_DIM), jnp.float32)
    scan_out = lax.scan(chunk_step, zero_state, chunk_inputs)
    y_heads = scan_out[1].reshape(SEQ_LEN, NUM_HEADS, HEAD_DIM) + d_skip[:, None] * xs_heads.reshape(SEQ_LEN, NUM_HEADS, HEAD_DIM).astype(jnp.float32)
    gated_y = y_heads.reshape(SEQ_LEN, NUM_GROUPS, GROUP_WIDTH) * jax.nn.silu(gate_in).reshape(SEQ_LEN, NUM_GROUPS, GROUP_WIDTH)
    normed = gated_y * lax.rsqrt(jnp.mean(gated_y * gated_y, axis=-1, keepdims=True) + NORM_EPS) * norm_w
    return jnp.dot(normed.reshape(SEQ_LEN, D_INNER).astype(jnp.bfloat16), w_out, preferred_element_type=jnp.float32).astype(jnp.bfloat16)
```

```python
import functools
import math

import jax
import jax.numpy as jnp
from jax import lax
from jax.experimental import pallas as pl
from jax.experimental.pallas import tpu as pltpu
from jax.sharding import PartitionSpec as P

CHUNK = 256
HALF = 128
EPS = 1e-5
LB = 512
LANES = 128
HALO = 16
ROWS = 64
LOG2E = math.log2(math.e)
MESH = pl.DeviceIdType.MESH
F32 = jnp.float32
BF16 = jnp.bfloat16


def dot(a, b):
    return jnp.dot(a, b, preferred_element_type=F32)


def dot_nt(a, b):
    return lax.dot_general(a, b, (((1,), (1,)), ((), ())), preferred_element_type=F32)


def split3(v):
    s1 = v.astype(BF16)
    r1 = v - s1.astype(F32)
    s2 = r1.astype(BF16)
    s3 = (r1 - s2.astype(F32)).astype(BF16)
    return s1, s2, s3


def half_silu(c):
    return c + c * jnp.tanh(c)


def mixer_kernel(dims, x_hbm, ds_ref, w_hbm, wdt_ref, cw_ref, cb_ref, dtb_ref, alog_ref, dsk_ref, nw_ref, g_hbm,
                 xe, wbuf, wbcd, zb, xb, yb, us, sc, cs0, tsend, two, tc, hrecv, hout, s0r, fbuf, soth,
                 bc, bt, gm, a2, apt, ldt, we, ws, arl, prm, dec, dpair, dchip, dg, mk, ssq, hal,
                 xsem, wsem, bsem, hs_sem, hr_sem, dp_sem, dps_sem, dg_sem, dgs_sem,
                 ps_sem, pr_sem, s1_sem, r1_sem, s2_sem, r2_sem, fs_sem, fr_sem, gsem):
    n_seq, n_tok, d_model, d_inner, n_heads, state_dim = dims
    head_dim = d_inner // n_heads
    nb = d_inner // LB
    hb = LB // head_dim
    npair = nb // 2
    n_chip = n_seq // 2
    hrows = state_dim // n_chip
    n_lt = LB // LANES
    n_zfirst = 2

    me = lax.axis_index('sp')
    chip = me // 2
    core = lax.rem(me, 2)
    partner = chip * 2 + (1 - core)

    def dev(i):
        return {'sp': i}

    def wcol(t):
        i2 = t - n_zfirst
        pair = i2 // 2
        own = lax.rem(i2, 2)
        ub = 2 * pair + jnp.where(own == 0, 1 - core, core)
        col = jnp.where(t < n_zfirst, t * LB,
                        jnp.where(t < n_zfirst + nb, d_inner + ub * LB, (t - nb) * LB))
        return pl.multiple_of(col, LB)

    def wcopy(t):
        slot = lax.rem(t, 3)
        return pltpu.make_async_copy(w_hbm.at[:, pl.ds(wcol(t), LB)], wbuf.at[slot], wsem.at[slot])

    n_steps = 2 * nb

    def wnext(t):
        wcopy(t).wait()

        @pl.when(t + 2 < n_steps)
        def _():
            wcopy(t + 2).start()

    xcopy = pltpu.make_async_copy(x_hbm, xe.at[pl.ds(HALO, n_tok)], xsem)
    xcopy.start()
    wcopy(jnp.int32(0)).start()
    bcopy = pltpu.make_async_copy(w_hbm.at[:, pl.ds(2 * d_inner, 2 * state_dim)], wbcd, bsem)
    bcopy.start()
    wcopy(jnp.int32(1)).start()

    barrier = pltpu.get_barrier_semaphore()
    pl.semaphore_signal(barrier, inc=1, device_id=dev(lax.rem(me + 1, n_seq)), device_id_type=MESH)
    pl.semaphore_signal(barrier, inc=1, device_id=dev(lax.rem(me + n_seq - 1, n_seq)), device_id_type=MESH)

    @pl.loop(1, n_chip)
    def _(r):
        pl.semaphore_signal(barrier, inc=1, device_id=dev(lax.rem(me + 2 * r, n_seq)), device_id_type=MESH)

    ri = lax.broadcasted_iota(jnp.int32, (CHUNK, CHUNK), 0)
    ci = lax.broadcasted_iota(jnp.int32, (CHUNK, CHUNK), 1)
    tri = (ri >= ci).astype(F32).astype(BF16)
    eye = (ri == ci).astype(F32).astype(BF16)
    n_chunks = n_tok // CHUNK
    per = CHUNK // LANES
    seg_cols, seg_rows, ds_cols = [], [], []
    for c in range(n_chunks):
        row = jnp.concatenate([ds_ref[per * c + q:per * c + q + 1, :] for q in range(per)], axis=1).astype(F32)
        row = jnp.broadcast_to(row, (8, CHUNK)).astype(BF16)
        ds_cols.append(jnp.broadcast_to(dot_nt(eye, row)[:, 0:1], (CHUNK, LANES)))
        seg_cols.append(jnp.broadcast_to(dot_nt(tri, row)[:, 0:1], (CHUNK, LANES)))
        seg_rows.append(dot_nt(row, tri)[0:1, :])
    keep = 1.0 - jnp.concatenate(ds_cols, axis=0)
    tok = lax.broadcasted_iota(jnp.int32, (n_tok, LANES), 0)
    m1 = keep
    k1 = jnp.where(tok >= 1, pltpu.roll(keep, 1, 0), 1.0)
    k2 = jnp.where(tok >= 2, pltpu.roll(keep, 2, 0), 1.0)
    mk[0] = m1
    mk[1] = m1 * k1
    mk[2] = m1 * k1 * k2

    xcopy.wait()
    hrow = lax.broadcasted_iota(jnp.int32, (HALO, LANES), 0)
    k_last = jnp.broadcast_to(mk[0, n_tok - 8:n_tok, :][7:8, :], (HALO, LANES))
    k_last2 = jnp.broadcast_to(mk[1, n_tok - 8:n_tok, :][7:8, :], (HALO, LANES))
    hmask = jnp.where(hrow == HALO - 1, 1.0, jnp.where(hrow == HALO - 2, k_last, jnp.where(hrow == HALO - 3, k_last2, 0.0)))
    for q in range(d_model // LANES):
        hal[:, q * LANES:(q + 1) * LANES] = (xe[n_tok:n_tok + HALO, q * LANES:(q + 1) * LANES].astype(F32) * hmask).astype(BF16)

    def zblock(t, zi):
        wnext(t)
        slot = lax.rem(t, 3)
        for q in range(n_tok // CHUNK):
            zb[zi, q * CHUNK:(q + 1) * CHUNK] = dot(xe[HALO + q * CHUNK:HALO + (q + 1) * CHUNK], wbuf[slot]).astype(BF16)

    pl.semaphore_wait(barrier, n_chip + 1)
    halo_send = pltpu.make_async_remote_copy(
        src_ref=hal, dst_ref=xe.at[pl.ds(0, HALO)], send_sem=hs_sem, recv_sem=hr_sem,
        device_id=dev(lax.rem(me + 1, n_seq)), device_id_type=MESH)

    @pl.when(me < n_seq - 1)
    def _():
        halo_send.start()

    @pl.when(me == 0)
    def _():
        xe[0:HALO, :] = jnp.zeros((HALO, d_model), BF16)

    @pl.loop(0, n_zfirst)
    def _(t):
        zblock(t, t)

    @pl.when(me > 0)
    def _():
        halo_send.wait_recv()

    bcopy.wait()
    mrow = (n_tok + HALO) // 3
    lane = lax.broadcasted_iota(jnp.int32, (1, LANES), 1)
    for q in range(3):
        us[q * mrow:(q + 1) * mrow, 0:2 * state_dim] = dot(xe[q * mrow:(q + 1) * mrow], wbcd[...]).astype(BF16).astype(F32)
        us[q * mrow:(q + 1) * mrow, 2 * state_dim:2 * state_dim + LANES] = dot(xe[q * mrow:(q + 1) * mrow], wdt_ref[...]).astype(BF16).astype(F32)

    def conv(r0, lt, wl):
        cols = slice(lt * LANES, (lt + 1) * LANES)
        ext = us[pl.ds(pl.multiple_of(r0 + HALO - 8, 8), ROWS + 8), cols]
        wl = pl.multiple_of(wl, LANES)
        cw = cw_ref[:, pl.ds(wl, LANES)] * 0.5
        v = cb_ref[:, pl.ds(wl, LANES)] * 0.5 + cw[0:1] * ext[8:8 + ROWS]
        for k in range(1, 4):
            v = v + cw[k:k + 1] * (mk[k - 1, pl.ds(r0, ROWS), :] * ext[8 - k:8 - k + ROWS])
        return half_silu(v)

    @pl.loop(0, n_tok // ROWS)
    def _(q):
        r0 = pl.multiple_of(q * ROWS, ROWS)
        for lt in range(2 * state_dim // LANES):
            bc[pl.ds(r0, ROWS), lt * LANES:(lt + 1) * LANES] = conv(r0, lt, d_inner + lt * LANES).astype(BF16)

    prm[...] = jnp.zeros((8, LANES), F32)
    prm[0:1, 0:n_heads] = dtb_ref[...]
    prm[1:2, 0:n_heads] = alog_ref[...]
    prm[2:3, 0:n_heads] = dsk_ref[...]
    pv = prm[...]
    head_ok = lane < n_heads
    neg_a = jnp.where(head_ok, -jnp.exp(pv[1:2]) , 0.0)
    e_rows = []
    for c in range(n_chunks):
        rows = slice(c * CHUNK, (c + 1) * CHUNK)
        raw = jnp.where(head_ok, us[HALO + c * CHUNK:HALO + (c + 1) * CHUNK, 2 * state_dim:2 * state_dim + LANES], 0.0) + pv[0:1]
        dt = jnp.maximum(raw, 0.0) + jnp.log1p(jnp.exp(-jnp.abs(raw)))
        s1, s2, s3 = split3(neg_a * dt * LOG2E)
        acum = dot(tri, s3) + dot(tri, s2) + dot(tri, s1)
        a2[rows, :] = acum
        a_t = jnp.transpose(acum)
        ld_t = jnp.transpose(jnp.log2(dt))
        ldt[:, rows] = ld_t
        apt[:, rows] = a_t - ld_t
        seg = seg_cols[c]
        last = acum[CHUNK - 1:CHUNK, :]
        seg_last = seg[CHUNK - 1:CHUNK, :]
        ws[rows, :] = jnp.where(seg == 0.0, jnp.exp2(acum), 0.0)
        we[rows, :] = jnp.where(seg == seg_last, jnp.exp2(last - acum) * dt, 0.0)
        e_rows.append(jnp.where(seg_last == 0.0, jnp.exp2(last), 0.0))
        b_c = bc[rows, 0:state_dim]
        c_c = bc[rows, state_dim:2 * state_dim]
        b_t = jnp.transpose(b_c.astype(F32)).astype(BF16)
        bt[c] = b_t
        scores = dot(c_c, b_t)
        same = jnp.concatenate([seg] * per, axis=1) == seg_rows[c]
        gm[c] = jnp.where(jnp.logical_and(ri >= ci, same), scores, 0.0)
    d_own = e_rows[0] * e_rows[1]
    dec[0:1, :] = e_rows[0]
    dec[1:2, :] = e_rows[1]
    dpair[core] = jnp.broadcast_to(d_own, (8, LANES))

    pair_send = pltpu.make_async_remote_copy(
        src_ref=dpair.at[core], dst_ref=dpair.at[core], send_sem=dps_sem, recv_sem=dp_sem,
        device_id=dev(partner), device_id_type=MESH)
    pair_send.start()
    pair_send.wait()
    dchip[...] = dpair[0] * dpair[1]
    dg[chip] = dpair[0] * dpair[1]
    dec[2:3, :] = dpair[0][0:1]
    dec[3:4, :] = dpair[1][0:1]

    @pl.loop(1, n_chip)
    def _(r):
        q = lax.rem(chip + r, n_chip)
        pltpu.make_async_remote_copy(
            src_ref=dchip, dst_ref=dg.at[chip], send_sem=dgs_sem, recv_sem=dg_sem,
            device_id=dev(2 * q + core), device_id_type=MESH).start()

    def expand(v, b):
        n = v.shape[0]
        r = pltpu.roll(v, lax.rem(2 * LANES - hb * b, LANES), 1)
        low = lax.broadcasted_iota(jnp.int32, (n, LANES), 1) < head_dim
        out = []
        for p in range(n_lt):
            out.append(jnp.where(low, jnp.broadcast_to(r[:, 2 * p:2 * p + 1], (n, LANES)),
                                 jnp.broadcast_to(r[:, 2 * p + 1:2 * p + 2], (n, LANES))))
        return jnp.concatenate(out, axis=1)

    def roll_to(dst, src, b):
        sh = lax.rem(2 * LANES - hb * b, LANES)
        for q in range(n_tok // LANES):
            dst[q * LANES:(q + 1) * LANES, :] = pltpu.roll(src[q * LANES:(q + 1) * LANES, :], sh, 1)

    low_r = lax.broadcasted_iota(jnp.int32, (ROWS, LANES), 1) < head_dim

    def head_cols(r0, lt):
        wv = arl[pl.ds(r0, ROWS), :]
        return jnp.where(low_r, jnp.broadcast_to(wv[:, 2 * lt:2 * lt + 1], (ROWS, LANES)),
                         jnp.broadcast_to(wv[:, 2 * lt + 1:2 * lt + 2], (ROWS, LANES)))

    def ublock(t, b, t_ref):
        wnext(t)
        slot = lax.rem(t, 3)
        for q in range(3):
            us[q * mrow:(q + 1) * mrow, :] = dot(xe[q * mrow:(q + 1) * mrow], wbuf[slot]).astype(BF16).astype(F32)
        roll_to(arl, we, b)

        @pl.loop(0, n_tok // ROWS)
        def _(q):
            r0 = pl.multiple_of(q * ROWS, ROWS)
            for lt in range(n_lt):
                cols = slice(lt * LANES, (lt + 1) * LANES)
                xs = conv(r0, lt, b * LB + lt * LANES).astype(BF16)
                xb[b, pl.ds(r0, ROWS), cols] = xs
                sc[pl.ds(r0, ROWS), cols] = (xs.astype(F32) * head_cols(r0, lt)).astype(BF16)

        ex = expand(dec[...], b)
        st0 = dot(bt[0], sc[0:CHUNK])
        cs0[b] = st0
        t_ref[...] = ex[1:2] * st0 + dot(bt[1], sc[CHUNK:2 * CHUNK])

    def part_copy(i):
        return pltpu.make_async_remote_copy(
            src_ref=tsend.at[i], dst_ref=two.at[i, core], send_sem=ps_sem.at[i], recv_sem=pr_sem.at[i],
            device_id=dev(partner), device_id_type=MESH)

    def home_copy(i, q):
        return pltpu.make_async_remote_copy(
            src_ref=tc.at[i, q], dst_ref=hrecv.at[i, chip], send_sem=s1_sem.at[i], recv_sem=r1_sem.at[i],
            device_id=dev(2 * q + core), device_id_type=MESH)

    def back_copy(i, q):
        return pltpu.make_async_remote_copy(
            src_ref=hout.at[i, q], dst_ref=s0r.at[i, chip], send_sem=s2_sem.at[i], recv_sem=r2_sem.at[i],
            device_id=dev(2 * q + core), device_id_type=MESH)

    def all_copies(src, dst, send_sem, recv_sem):
        return pltpu.make_async_remote_copy(
            src_ref=src.at[pl.ds(0, n_chip - 1)], dst_ref=dst.at[pl.ds(0, n_chip - 1)], send_sem=send_sem, recv_sem=recv_sem,
            device_id=dev(partner), device_id_type=MESH)

    def fin_copy(i):
        return pltpu.make_async_remote_copy(
            src_ref=fbuf.at[i, 1 - core], dst_ref=soth.at[i], send_sem=fs_sem.at[i], recv_sem=fr_sem.at[i],
            device_id=dev(partner), device_id_type=MESH)

    def send_home(i, b):
        part_copy(i).wait_recv()
        ex = expand(dec[...], b)
        for q in range(n_chip):
            rows = slice(q * hrows, (q + 1) * hrows)
            tc[i, q] = ex[3:4] * two[i, 0, rows] + two[i, 1, rows]
        hrecv[i, chip] = tc[i, chip]

        @pl.loop(1, n_chip)
        def _(r):
            home_copy(i, lax.rem(chip + r, n_chip)).start()

    def home(i):
        b = 2 * i + core
        all_copies(tc.at[i], hrecv.at[i], s1_sem.at[i], r1_sem.at[i]).wait_recv()
        run = jnp.zeros((hrows, LB), F32)
        for q in range(n_chip):
            hout[i, q] = run
            run = expand(dg[q], b)[0:1] * run + hrecv[i, q]
        s0r[i, chip] = hout[i, chip]

        @pl.loop(1, n_chip)
        def _(r):
            back_copy(i, lax.rem(chip + r, n_chip)).start()

    def finish(i):
        b = 2 * i + core
        all_copies(hout.at[i], s0r.at[i], s2_sem.at[i], r2_sem.at[i]).wait_recv()
        ex = expand(dec[...], b)
        for q in range(n_chip):
            rows = slice(q * hrows, (q + 1) * hrows)
            fbuf[i, 0, rows] = s0r[i, q]
            fbuf[i, 1, rows] = ex[2:3] * s0r[i, q] + two[i, 0, rows]
        fin_copy(i).start()

    @pl.loop(0, npair)
    def _(i):
        t = n_zfirst + 2 * i
        ublock(t, 2 * i + 1 - core, tsend.at[i])
        part_copy(i).start()
        ublock(t + 1, 2 * i + core, two.at[i, core])
        send_home(i, 2 * i + core)

        @pl.when(i == 0)
        def _():
            all_copies(dg, dg, dgs_sem, dg_sem).wait_recv()

        @pl.when(i >= 1)
        def _():
            home(i - 1)

        @pl.when(i >= 2)
        def _():
            finish(i - 2)

    low_b = (lax.broadcasted_iota(jnp.int32, (CHUNK, LANES), 1) < head_dim).astype(F32).astype(BF16)
    high_b = (lax.broadcasted_iota(jnp.int32, (CHUNK, LANES), 1) >= head_dim).astype(F32).astype(BF16)

    def intra(b):
        roll_to(arl, a2, b)
        hrows8 = pl.ds(pl.multiple_of(b * hb, hb), hb)
        dsk = expand(prm[...], b)[2:3]
        for c in range(n_chunks):
            r0 = c * CHUNK
            for p in range(n_lt):
                cols = slice(p * LANES, (p + 1) * LANES)
                lhs0, lhs1 = [], []
                for h in (2 * p, 2 * p + 1):
                    ai0 = jnp.broadcast_to(arl[r0:r0 + HALF, h:h + 1], (HALF, HALF))
                    ai1 = jnp.broadcast_to(arl[r0 + HALF:r0 + CHUNK, h:h + 1], (HALF, HALF))
                    aj = apt[hrows8, r0:r0 + CHUNK][h:h + 1]
                    ld = ldt[hrows8, r0:r0 + CHUNK][h:h + 1]
                    lhs0.append((jnp.exp2(jnp.minimum(ai0 - aj[:, :HALF], ld[:, :HALF])) * gm[c, 0:HALF, 0:HALF]).astype(BF16))
                    lhs1.append((jnp.exp2(ai1 - aj[:, :HALF]) * gm[c, HALF:CHUNK, 0:HALF]).astype(BF16))
                    lhs1.append((jnp.exp2(jnp.minimum(ai1 - aj[:, HALF:], ld[:, HALF:])) * gm[c, HALF:CHUNK, HALF:CHUNK]).astype(BF16))
                xp = xb[b, r0:r0 + CHUNK, cols]
                xa, xh = xp * low_b, xp * high_b
                y0 = dot(jnp.concatenate(lhs0, axis=1), jnp.concatenate([xa[:HALF], xh[:HALF]], axis=0))
                y1 = dot(jnp.concatenate(lhs1, axis=1), jnp.concatenate([xa, xh], axis=0))
                yb[b, r0:r0 + HALF, cols] = y0 + dsk[:, cols] * xp[:HALF].astype(F32)
                yb[b, r0 + HALF:r0 + CHUNK, cols] = y1 + dsk[:, cols] * xp[HALF:].astype(F32)

    @pl.loop(0, nb)
    def _(m):
        intra(m)

        @pl.when(m < nb - n_zfirst)
        def _():
            zblock(m + n_zfirst + nb, m + n_zfirst)

        @pl.when(m == 0)
        def _():
            home(npair - 1)

        @pl.when(m == 1)
        def _():
            finish(npair - 2)

        @pl.when(m == nb - 5)
        def _():
            finish(npair - 1)

    ssq[...] = jnp.zeros((n_tok, LANES), F32)

    def close(b, s_ref):
        ex = expand(dec[...], b)
        roll_to(arl, ws, b)
        s_in = s_ref[...]
        us[0:CHUNK, :] = dot(bc[0:CHUNK, state_dim:2 * state_dim], s_in.astype(BF16))
        s_mid = ex[0:1] * s_in + cs0[b]
        us[CHUNK:2 * CHUNK, :] = dot(bc[CHUNK:2 * CHUNK, state_dim:2 * state_dim], s_mid.astype(BF16))

        @pl.loop(0, n_tok // ROWS)
        def _(q):
            rows = pl.ds(pl.multiple_of(q * ROWS, ROWS), ROWS)
            acc = ssq[rows, :]
            for lt in range(n_lt):
                cols = slice(lt * LANES, (lt + 1) * LANES)
                y = yb[b, rows, cols] + head_cols(q * ROWS, lt) * us[rows, cols]
                gated = y * half_silu(zb[b, rows, cols].astype(F32) * 0.5)
                yb[b, rows, cols] = gated
                acc = acc + gated * gated
            ssq[rows, :] = acc

    @pl.loop(0, npair)
    def _(i):
        close(2 * i + core, fbuf.at[i, core])
        fin_copy(i).wait_recv()
        close(2 * i + 1 - core, soth.at[i])

    scale = lax.rsqrt(jnp.sum(ssq[...], axis=1, keepdims=True) * (1.0 / d_inner) + EPS)
    ssq[...] = jnp.broadcast_to(scale, (n_tok, LANES))

    def gcopy(b):
        return pltpu.make_async_copy(zb.at[b], g_hbm.at[:, pl.ds(pl.multiple_of(b * LB, LB), LB)], gsem.at[b])

    @pl.loop(0, nb)
    def _(b):
        @pl.loop(0, n_tok // ROWS)
        def _(q):
            rows = pl.ds(pl.multiple_of(q * ROWS, ROWS), ROWS)
            sv = ssq[rows, :]
            for lt in range(n_lt):
                cols = slice(lt * LANES, (lt + 1) * LANES)
                nw = nw_ref[:, pl.ds(pl.multiple_of(b * LB + lt * LANES, LANES), LANES)]
                zb[b, rows, cols] = (yb[b, rows, cols] * sv * nw).astype(BF16)
        gcopy(b).start()

    @pl.when(me < n_seq - 1)
    def _():
        halo_send.wait_send()

    all_copies(dg, dg, dgs_sem, dg_sem).wait_send()

    @pl.loop(0, npair)
    def _(i):
        part_copy(i).wait_send()
        all_copies(tc.at[i], hrecv.at[i], s1_sem.at[i], r1_sem.at[i]).wait_send()
        all_copies(hout.at[i], s0r.at[i], s2_sem.at[i], r2_sem.at[i]).wait_send()
        fin_copy(i).wait_send()

    @pl.loop(0, nb)
    def _(b):
        gcopy(b).wait()


def mixer(n_seq, x, doc_start, w_in, conv_w, conv_b, dt_bias, a_log, d_skip, norm_w):
    n_tok, d_model = x.shape
    d_inner = norm_w.shape[0] * norm_w.shape[1]
    n_heads = a_log.shape[0]
    state_dim = (conv_w.shape[1] - d_inner) // 2
    nb = d_inner // LB
    npair = nb // 2
    n_chip = n_seq // 2
    hrows = state_dim // n_chip
    dims = (n_seq, n_tok, d_model, d_inner, n_heads, state_dim)
    dt_block = (2 * d_inner + 2 * state_dim) // LANES
    vmem = pl.BlockSpec(memory_space=pltpu.VMEM)
    anyspace = pl.BlockSpec(memory_space=pl.ANY)
    dma = pltpu.SemaphoreType.DMA
    scratch = [
        pltpu.VMEM((n_tok + HALO, d_model), BF16),
        pltpu.VMEM((3, d_model, LB), BF16),
        pltpu.VMEM((d_model, 2 * state_dim), BF16),
        pltpu.VMEM((nb, n_tok, LB), BF16),
        pltpu.VMEM((nb, n_tok, LB), BF16),
        pltpu.VMEM((nb, n_tok, LB), F32),
        pltpu.VMEM((n_tok + HALO, LB), F32),
        pltpu.VMEM((n_tok, LB), BF16),
        pltpu.VMEM((nb, state_dim, LB), F32),
        pltpu.VMEM((npair, state_dim, LB), F32),
        pltpu.VMEM((npair, 2, state_dim, LB), F32),
        pltpu.VMEM((npair, n_chip, hrows, LB), F32),
        pltpu.VMEM((npair, n_chip, hrows, LB), F32),
        pltpu.VMEM((npair, n_chip, hrows, LB), F32),
        pltpu.VMEM((npair, n_chip, hrows, LB), F32),
        pltpu.VMEM((npair, 2, state_dim, LB), F32),
        pltpu.VMEM((npair, state_dim, LB), F32),
        pltpu.VMEM((n_tok, 2 * state_dim), BF16),
        pltpu.VMEM((n_tok // CHUNK, state_dim, CHUNK), BF16),
        pltpu.VMEM((n_tok // CHUNK, CHUNK, CHUNK), F32),
        pltpu.VMEM((n_tok, LANES), F32),
        pltpu.VMEM((LANES, n_tok), F32),
        pltpu.VMEM((LANES, n_tok), F32),
        pltpu.VMEM((n_tok, LANES), F32),
        pltpu.VMEM((n_tok, LANES), F32),
        pltpu.VMEM((n_tok, LANES), F32),
        pltpu.VMEM((8, LANES), F32),
        pltpu.VMEM((8, LANES), F32),
        pltpu.VMEM((2, 8, LANES), F32),
        pltpu.VMEM((8, LANES), F32),
        pltpu.VMEM((n_chip, 8, LANES), F32),
        pltpu.VMEM((3, n_tok, LANES), F32),
        pltpu.VMEM((n_tok, LANES), F32),
        pltpu.VMEM((HALO, d_model), BF16),
        dma(()), dma((3,)), dma(()), dma(()), dma(()), dma(()), dma(()), dma(()), dma(()),
        dma((npair,)), dma((npair,)), dma((npair,)), dma((npair,)), dma((npair,)), dma((npair,)), dma((npair,)), dma((npair,)),
        dma((nb,)),
    ]
    return pl.pallas_call(
        functools.partial(mixer_kernel, dims),
        out_shape=jax.ShapeDtypeStruct((n_tok, d_inner), BF16),
        grid=(1,),
        in_specs=[anyspace, vmem, anyspace, pl.BlockSpec((d_model, LANES), lambda i: (0, dt_block), pipeline_mode=pl.Buffered(1)), vmem, vmem, vmem, vmem, vmem, vmem],
        out_specs=anyspace,
        scratch_shapes=scratch,
        compiler_params=pltpu.CompilerParams(collective_id=0, has_side_effects=True, vmem_limit_bytes=66 * 1000 * 1000),
        name='mixer',
    )(x, doc_start.reshape(n_tok // LANES, LANES), w_in, w_in, conv_w, conv_b.reshape(1, -1), dt_bias.reshape(1, -1),
      a_log.reshape(1, -1), d_skip.reshape(1, -1), norm_w.reshape(1, -1))


def solution(mesh):
    n_seq = mesh.shape['sp']
    row_spec = P(('dp', 'sp'), None)
    tok_spec = P(('dp', 'sp'))

    def layer_shard(x, doc_start, w_in, conv_w, conv_b, dt_bias, a_log, d_skip, norm_w, w_out):
        g = mixer(n_seq, x, doc_start, w_in, conv_w, conv_b, dt_bias, a_log, d_skip, norm_w)
        return jnp.dot(g, w_out, preferred_element_type=F32).astype(BF16)

    return jax.shard_map(layer_shard, mesh=mesh, in_specs=(row_spec, tok_spec, P(), P(), P(), P(), P(), P(), P(), P()), out_specs=row_spec, check_vma=False)
```

```python
import functools
import math

import jax
import jax.numpy as jnp
from jax import lax
from jax.experimental import pallas as pl
from jax.experimental.pallas import tpu as pltpu
from jax.sharding import PartitionSpec as P

CHUNK = 256
HALF = 128
EPS = 1e-5
LB = 512
LANES = 128
HALO = 16
ROWS = 64
LOG2E = math.log2(math.e)
MESH = pl.DeviceIdType.MESH
F32 = jnp.float32
BF16 = jnp.bfloat16


def dot(a, b):
    return jnp.dot(a, b, preferred_element_type=F32)


def dot_nt(a, b):
    return lax.dot_general(a, b, (((1,), (1,)), ((), ())), preferred_element_type=F32)


def split3(v):
    s1 = v.astype(BF16)
    r1 = v - s1.astype(F32)
    s2 = r1.astype(BF16)
    s3 = (r1 - s2.astype(F32)).astype(BF16)
    return s1, s2, s3


def half_silu(c):
    return c + c * jnp.tanh(c)


def mixer_kernel(dims, x_hbm, ds_ref, w_hbm, cw_ref, cb_ref, dtb_ref, alog_ref, dsk_ref, nw_ref, g_hbm,
                 xe, wbuf, wbcd, zb, xb, yb, us, sc, cs0, tsend, two, tc, hrecv, hout, s0r, fbuf, soth,
                 bc, bt, gm, a2, apt, ldt, we, ws, arl, prm, dec, dpair, dchip, dg, mk, ssq, hal,
                 xsem, wsem, bsem, hs_sem, hr_sem, dp_sem, dps_sem, dg_sem, dgs_sem,
                 ps_sem, pr_sem, s1_sem, r1_sem, s2_sem, r2_sem, fs_sem, fr_sem, gsem):
    n_seq, n_tok, d_model, d_inner, n_heads, state_dim = dims
    head_dim = d_inner // n_heads
    nb = d_inner // LB
    hb = LB // head_dim
    npair = nb // 2
    n_chip = n_seq // 2
    hrows = state_dim // n_chip
    n_bcd = 2 * state_dim + n_heads
    n_lt = LB // LANES
    n_zfirst = 2

    me = lax.axis_index('sp')
    chip = me // 2
    core = lax.rem(me, 2)
    partner = chip * 2 + (1 - core)

    def dev(i):
        return {'sp': i}

    def wcol(t):
        i2 = t - n_zfirst
        pair = i2 // 2
        own = lax.rem(i2, 2)
        ub = 2 * pair + jnp.where(own == 0, 1 - core, core)
        col = jnp.where(t < n_zfirst, t * LB,
                        jnp.where(t < n_zfirst + nb, d_inner + ub * LB, (t - nb) * LB))
        return pl.multiple_of(col, LB)

    def wcopy(t):
        slot = lax.rem(t, 3)
        return pltpu.make_async_copy(w_hbm.at[pl.ds(wcol(t), LB)], wbuf.at[slot], wsem.at[slot])

    n_steps = 2 * nb

    def wnext(t):
        wcopy(t).wait()

        @pl.when(t + 2 < n_steps)
        def _():
            wcopy(t + 2).start()

    xcopy = pltpu.make_async_copy(x_hbm, xe.at[pl.ds(HALO, n_tok)], xsem)
    xcopy.start()
    wcopy(jnp.int32(0)).start()
    bcopy = pltpu.make_async_copy(w_hbm.at[pl.ds(2 * d_inner, n_bcd)], wbcd.at[pl.ds(0, n_bcd)], bsem)
    bcopy.start()
    wbcd[n_bcd:, :] = jnp.zeros((LANES - n_heads, d_model), BF16)
    wcopy(jnp.int32(1)).start()

    barrier = pltpu.get_barrier_semaphore()
    pl.semaphore_signal(barrier, inc=1, device_id=dev(lax.rem(me + 1, n_seq)), device_id_type=MESH)
    pl.semaphore_signal(barrier, inc=1, device_id=dev(lax.rem(me + n_seq - 1, n_seq)), device_id_type=MESH)

    @pl.loop(1, n_chip)
    def _(r):
        pl.semaphore_signal(barrier, inc=1, device_id=dev(lax.rem(me + 2 * r, n_seq)), device_id_type=MESH)

    ri = lax.broadcasted_iota(jnp.int32, (CHUNK, CHUNK), 0)
    ci = lax.broadcasted_iota(jnp.int32, (CHUNK, CHUNK), 1)
    tri = (ri >= ci).astype(F32).astype(BF16)
    eye = (ri == ci).astype(F32).astype(BF16)
    n_chunks = n_tok // CHUNK
    per = CHUNK // LANES
    seg_cols, seg_rows, ds_cols = [], [], []
    for c in range(n_chunks):
        row = jnp.concatenate([ds_ref[per * c + q:per * c + q + 1, :] for q in range(per)], axis=1).astype(F32)
        row = jnp.broadcast_to(row, (8, CHUNK)).astype(BF16)
        ds_cols.append(jnp.broadcast_to(dot_nt(eye, row)[:, 0:1], (CHUNK, LANES)))
        seg_cols.append(jnp.broadcast_to(dot_nt(tri, row)[:, 0:1], (CHUNK, LANES)))
        seg_rows.append(dot_nt(row, tri)[0:1, :])
    keep = 1.0 - jnp.concatenate(ds_cols, axis=0)
    tok = lax.broadcasted_iota(jnp.int32, (n_tok, LANES), 0)
    m1 = keep
    k1 = jnp.where(tok >= 1, pltpu.roll(keep, 1, 0), 1.0)
    k2 = jnp.where(tok >= 2, pltpu.roll(keep, 2, 0), 1.0)
    mk[0] = m1
    mk[1] = m1 * k1
    mk[2] = m1 * k1 * k2

    xcopy.wait()
    hrow = lax.broadcasted_iota(jnp.int32, (HALO, LANES), 0)
    k_last = jnp.broadcast_to(mk[0, n_tok - 8:n_tok, :][7:8, :], (HALO, LANES))
    k_last2 = jnp.broadcast_to(mk[1, n_tok - 8:n_tok, :][7:8, :], (HALO, LANES))
    hmask = jnp.where(hrow == HALO - 1, 1.0, jnp.where(hrow == HALO - 2, k_last, jnp.where(hrow == HALO - 3, k_last2, 0.0)))
    for q in range(d_model // LANES):
        hal[:, q * LANES:(q + 1) * LANES] = (xe[n_tok:n_tok + HALO, q * LANES:(q + 1) * LANES].astype(F32) * hmask).astype(BF16)

    def zblock(t, zi):
        wnext(t)
        slot = lax.rem(t, 3)
        for q in range(n_tok // CHUNK):
            zb[zi, q * CHUNK:(q + 1) * CHUNK] = dot_nt(xe[HALO + q * CHUNK:HALO + (q + 1) * CHUNK], wbuf[slot]).astype(BF16)

    pl.semaphore_wait(barrier, n_chip + 1)
    halo_send = pltpu.make_async_remote_copy(
        src_ref=hal, dst_ref=xe.at[pl.ds(0, HALO)], send_sem=hs_sem, recv_sem=hr_sem,
        device_id=dev(lax.rem(me + 1, n_seq)), device_id_type=MESH)

    @pl.when(me < n_seq - 1)
    def _():
        halo_send.start()

    @pl.when(me == 0)
    def _():
        xe[0:HALO, :] = jnp.zeros((HALO, d_model), BF16)

    @pl.loop(0, n_zfirst)
    def _(t):
        zblock(t, t)

    @pl.when(me > 0)
    def _():
        halo_send.wait_recv()

    bcopy.wait()
    mrow = (n_tok + HALO) // 2
    lane = lax.broadcasted_iota(jnp.int32, (1, LANES), 1)
    for q in range(2):
        us[q * mrow:(q + 1) * mrow, 0:2 * state_dim + LANES] = dot_nt(xe[q * mrow:(q + 1) * mrow], wbcd[...]).astype(BF16).astype(F32)

    def conv(r0, lt, wl):
        cols = slice(lt * LANES, (lt + 1) * LANES)
        ext = us[pl.ds(pl.multiple_of(r0 + HALO - 8, 8), ROWS + 8), cols]
        wl = pl.multiple_of(wl, LANES)
        cw = cw_ref[:, pl.ds(wl, LANES)] * 0.5
        v = cb_ref[:, pl.ds(wl, LANES)] * 0.5 + cw[0:1] * ext[8:8 + ROWS]
        for k in range(1, 4):
            v = v + cw[k:k + 1] * (mk[k - 1, pl.ds(r0, ROWS), :] * ext[8 - k:8 - k + ROWS])
        return half_silu(v)

    @pl.loop(0, n_tok // ROWS)
    def _(q):
        r0 = pl.multiple_of(q * ROWS, ROWS)
        for lt in range(2 * state_dim // LANES):
            bc[pl.ds(r0, ROWS), lt * LANES:(lt + 1) * LANES] = conv(r0, lt, d_inner + lt * LANES).astype(BF16)

    prm[...] = jnp.zeros((8, LANES), F32)
    prm[0:1, 0:n_heads] = dtb_ref[...]
    prm[1:2, 0:n_heads] = alog_ref[...]
    prm[2:3, 0:n_heads] = dsk_ref[...]
    pv = prm[...]
    head_ok = lane < n_heads
    neg_a = jnp.where(head_ok, -jnp.exp(pv[1:2]) , 0.0)
    e_rows = []
    for c in range(n_chunks):
        rows = slice(c * CHUNK, (c + 1) * CHUNK)
        raw = jnp.where(head_ok, us[HALO + c * CHUNK:HALO + (c + 1) * CHUNK, 2 * state_dim:2 * state_dim + LANES], 0.0) + pv[0:1]
        dt = jnp.maximum(raw, 0.0) + jnp.log1p(jnp.exp(-jnp.abs(raw)))
        s1, s2, s3 = split3(neg_a * dt * LOG2E)
        acum = dot(tri, s3) + dot(tri, s2) + dot(tri, s1)
        a2[rows, :] = acum
        a_t = jnp.transpose(acum)
        ld_t = jnp.transpose(jnp.log2(dt))
        ldt[:, rows] = ld_t
        apt[:, rows] = a_t - ld_t
        seg = seg_cols[c]
        last = acum[CHUNK - 1:CHUNK, :]
        seg_last = seg[CHUNK - 1:CHUNK, :]
        ws[rows, :] = jnp.where(seg == 0.0, jnp.exp2(acum), 0.0)
        we[rows, :] = jnp.where(seg == seg_last, jnp.exp2(last - acum) * dt, 0.0)
        e_rows.append(jnp.where(seg_last == 0.0, jnp.exp2(last), 0.0))
        b_c = bc[rows, 0:state_dim]
        c_c = bc[rows, state_dim:2 * state_dim]
        b_t = jnp.transpose(b_c.astype(F32)).astype(BF16)
        bt[c] = b_t
        scores = dot(c_c, b_t)
        same = jnp.concatenate([seg] * per, axis=1) == seg_rows[c]
        gm[c] = jnp.where(jnp.logical_and(ri >= ci, same), scores, 0.0)
    d_own = e_rows[0] * e_rows[1]
    dec[0:1, :] = e_rows[0]
    dec[1:2, :] = e_rows[1]
    dpair[core] = jnp.broadcast_to(d_own, (8, LANES))

    pair_send = pltpu.make_async_remote_copy(
        src_ref=dpair.at[core], dst_ref=dpair.at[core], send_sem=dps_sem, recv_sem=dp_sem,
        device_id=dev(partner), device_id_type=MESH)
    pair_send.start()
    pair_send.wait()
    dchip[...] = dpair[0] * dpair[1]
    dg[chip] = dpair[0] * dpair[1]
    dec[2:3, :] = dpair[0][0:1]
    dec[3:4, :] = dpair[1][0:1]

    @pl.loop(1, n_chip)
    def _(r):
        q = lax.rem(chip + r, n_chip)
        pltpu.make_async_remote_copy(
            src_ref=dchip, dst_ref=dg.at[chip], send_sem=dgs_sem, recv_sem=dg_sem,
            device_id=dev(2 * q + core), device_id_type=MESH).start()

    def expand(v, b):
        n = v.shape[0]
        r = pltpu.roll(v, lax.rem(2 * LANES - hb * b, LANES), 1)
        low = lax.broadcasted_iota(jnp.int32, (n, LANES), 1) < head_dim
        out = []
        for p in range(n_lt):
            out.append(jnp.where(low, jnp.broadcast_to(r[:, 2 * p:2 * p + 1], (n, LANES)),
                                 jnp.broadcast_to(r[:, 2 * p + 1:2 * p + 2], (n, LANES))))
        return jnp.concatenate(out, axis=1)

    def roll_to(dst, src, b):
        sh = lax.rem(2 * LANES - hb * b, LANES)
        for q in range(n_tok // LANES):
            dst[q * LANES:(q + 1) * LANES, :] = pltpu.roll(src[q * LANES:(q + 1) * LANES, :], sh, 1)

    low_r = lax.broadcasted_iota(jnp.int32, (ROWS, LANES), 1) < head_dim

    def head_cols(r0, lt):
        wv = arl[pl.ds(r0, ROWS), :]
        return jnp.where(low_r, jnp.broadcast_to(wv[:, 2 * lt:2 * lt + 1], (ROWS, LANES)),
                         jnp.broadcast_to(wv[:, 2 * lt + 1:2 * lt + 2], (ROWS, LANES)))

    def ublock(t, b, t_ref):
        wnext(t)
        slot = lax.rem(t, 3)
        for q in range(2):
            us[q * mrow:(q + 1) * mrow, :] = dot_nt(xe[q * mrow:(q + 1) * mrow], wbuf[slot]).astype(BF16).astype(F32)
        roll_to(arl, we, b)

        @pl.loop(0, n_tok // ROWS)
        def _(q):
            r0 = pl.multiple_of(q * ROWS, ROWS)
            for lt in range(n_lt):
                cols = slice(lt * LANES, (lt + 1) * LANES)
                xs = conv(r0, lt, b * LB + lt * LANES).astype(BF16)
                xb[b, pl.ds(r0, ROWS), cols] = xs
                sc[pl.ds(r0, ROWS), cols] = (xs.astype(F32) * head_cols(r0, lt)).astype(BF16)

        ex = expand(dec[...], b)
        st0 = dot(bt[0], sc[0:CHUNK])
        cs0[b] = st0
        t_ref[...] = ex[1:2] * st0 + dot(bt[1], sc[CHUNK:2 * CHUNK])

    def part_copy(i):
        return pltpu.make_async_remote_copy(
            src_ref=tsend.at[i], dst_ref=two.at[i, core], send_sem=ps_sem.at[i], recv_sem=pr_sem.at[i],
            device_id=dev(partner), device_id_type=MESH)

    def home_copy(i, q):
        return pltpu.make_async_remote_copy(
            src_ref=tc.at[i, q], dst_ref=hrecv.at[i, chip], send_sem=s1_sem.at[i], recv_sem=r1_sem.at[i],
            device_id=dev(2 * q + core), device_id_type=MESH)

    def back_copy(i, q):
        return pltpu.make_async_remote_copy(
            src_ref=hout.at[i, q], dst_ref=s0r.at[i, chip], send_sem=s2_sem.at[i], recv_sem=r2_sem.at[i],
            device_id=dev(2 * q + core), device_id_type=MESH)

    def all_copies(src, dst, send_sem, recv_sem):
        return pltpu.make_async_remote_copy(
            src_ref=src.at[pl.ds(0, n_chip - 1)], dst_ref=dst.at[pl.ds(0, n_chip - 1)], send_sem=send_sem, recv_sem=recv_sem,
            device_id=dev(partner), device_id_type=MESH)

    def fin_copy(i):
        return pltpu.make_async_remote_copy(
            src_ref=fbuf.at[i, 1 - core], dst_ref=soth.at[i], send_sem=fs_sem.at[i], recv_sem=fr_sem.at[i],
            device_id=dev(partner), device_id_type=MESH)

    def send_home(i, b):
        part_copy(i).wait_recv()
        ex = expand(dec[...], b)
        for q in range(n_chip):
            rows = slice(q * hrows, (q + 1) * hrows)
            tc[i, q] = ex[3:4] * two[i, 0, rows] + two[i, 1, rows]
        hrecv[i, chip] = tc[i, chip]

        @pl.loop(1, n_chip)
        def _(r):
            home_copy(i, lax.rem(chip + r, n_chip)).start()

    def home(i):
        b = 2 * i + core
        all_copies(tc.at[i], hrecv.at[i], s1_sem.at[i], r1_sem.at[i]).wait_recv()
        run = jnp.zeros((hrows, LB), F32)
        for q in range(n_chip):
            hout[i, q] = run
            run = expand(dg[q], b)[0:1] * run + hrecv[i, q]
        s0r[i, chip] = hout[i, chip]

        @pl.loop(1, n_chip)
        def _(r):
            back_copy(i, lax.rem(chip + r, n_chip)).start()

    def finish(i):
        b = 2 * i + core
        all_copies(hout.at[i], s0r.at[i], s2_sem.at[i], r2_sem.at[i]).wait_recv()
        ex = expand(dec[...], b)
        for q in range(n_chip):
            rows = slice(q * hrows, (q + 1) * hrows)
            fbuf[i, 0, rows] = s0r[i, q]
            fbuf[i, 1, rows] = ex[2:3] * s0r[i, q] + two[i, 0, rows]
        fin_copy(i).start()

    @pl.loop(0, npair)
    def _(i):
        t = n_zfirst + 2 * i
        ublock(t, 2 * i + 1 - core, tsend.at[i])
        part_copy(i).start()
        ublock(t + 1, 2 * i + core, two.at[i, core])
        send_home(i, 2 * i + core)

        @pl.when(i == 0)
        def _():
            all_copies(dg, dg, dgs_sem, dg_sem).wait_recv()

        @pl.when(i >= 1)
        def _():
            home(i - 1)

        @pl.when(i >= 2)
        def _():
            finish(i - 2)

    low_b = (lax.broadcasted_iota(jnp.int32, (CHUNK, LANES), 1) < head_dim).astype(F32).astype(BF16)
    high_b = (lax.broadcasted_iota(jnp.int32, (CHUNK, LANES), 1) >= head_dim).astype(F32).astype(BF16)

    def intra(b):
        roll_to(arl, a2, b)
        hrows8 = pl.ds(pl.multiple_of(b * hb, hb), hb)
        dsk = expand(prm[...], b)[2:3]
        for c in range(n_chunks):
            r0 = c * CHUNK
            for p in range(n_lt):
                cols = slice(p * LANES, (p + 1) * LANES)
                lhs0, lhs1 = [], []
                for h in (2 * p, 2 * p + 1):
                    ai0 = jnp.broadcast_to(arl[r0:r0 + HALF, h:h + 1], (HALF, HALF))
                    ai1 = jnp.broadcast_to(arl[r0 + HALF:r0 + CHUNK, h:h + 1], (HALF, HALF))
                    aj = apt[hrows8, r0:r0 + CHUNK][h:h + 1]
                    ld = ldt[hrows8, r0:r0 + CHUNK][h:h + 1]
                    lhs0.append((jnp.exp2(jnp.minimum(ai0 - aj[:, :HALF], ld[:, :HALF])) * gm[c, 0:HALF, 0:HALF]).astype(BF16))
                    lhs1.append((jnp.exp2(ai1 - aj[:, :HALF]) * gm[c, HALF:CHUNK, 0:HALF]).astype(BF16))
                    lhs1.append((jnp.exp2(jnp.minimum(ai1 - aj[:, HALF:], ld[:, HALF:])) * gm[c, HALF:CHUNK, HALF:CHUNK]).astype(BF16))
                xp = xb[b, r0:r0 + CHUNK, cols]
                xa, xh = xp * low_b, xp * high_b
                y0 = dot(jnp.concatenate(lhs0, axis=1), jnp.concatenate([xa[:HALF], xh[:HALF]], axis=0))
                y1 = dot(jnp.concatenate(lhs1, axis=1), jnp.concatenate([xa, xh], axis=0))
                yb[b, r0:r0 + HALF, cols] = y0 + dsk[:, cols] * xp[:HALF].astype(F32)
                yb[b, r0 + HALF:r0 + CHUNK, cols] = y1 + dsk[:, cols] * xp[HALF:].astype(F32)

    @pl.loop(0, nb)
    def _(m):
        intra(m)

        @pl.when(m < nb - n_zfirst)
        def _():
            zblock(m + n_zfirst + nb, m + n_zfirst)

        @pl.when(m == 0)
        def _():
            home(npair - 1)

        @pl.when(m == 1)
        def _():
            finish(npair - 2)

        @pl.when(m == nb - 5)
        def _():
            finish(npair - 1)

    ssq[...] = jnp.zeros((n_tok, LANES), F32)

    def close(b, s_ref):
        ex = expand(dec[...], b)
        roll_to(arl, ws, b)
        s_in = s_ref[...]
        us[0:CHUNK, :] = dot(bc[0:CHUNK, state_dim:2 * state_dim], s_in.astype(BF16))
        s_mid = ex[0:1] * s_in + cs0[b]
        us[CHUNK:2 * CHUNK, :] = dot(bc[CHUNK:2 * CHUNK, state_dim:2 * state_dim], s_mid.astype(BF16))

        @pl.loop(0, n_tok // ROWS)
        def _(q):
            rows = pl.ds(pl.multiple_of(q * ROWS, ROWS), ROWS)
            acc = ssq[rows, :]
            for lt in range(n_lt):
                cols = slice(lt * LANES, (lt + 1) * LANES)
                y = yb[b, rows, cols] + head_cols(q * ROWS, lt) * us[rows, cols]
                gated = y * half_silu(zb[b, rows, cols].astype(F32) * 0.5)
                yb[b, rows, cols] = gated
                acc = acc + gated * gated
            ssq[rows, :] = acc

    @pl.loop(0, npair)
    def _(i):
        close(2 * i + core, fbuf.at[i, core])
        fin_copy(i).wait_recv()
        close(2 * i + 1 - core, soth.at[i])

    scale = lax.rsqrt(jnp.sum(ssq[...], axis=1, keepdims=True) * (1.0 / d_inner) + EPS)
    ssq[...] = jnp.broadcast_to(scale, (n_tok, LANES))

    def gcopy(b):
        return pltpu.make_async_copy(zb.at[b], g_hbm.at[:, pl.ds(pl.multiple_of(b * LB, LB), LB)], gsem.at[b])

    @pl.loop(0, nb)
    def _(b):
        @pl.loop(0, n_tok // ROWS)
        def _(q):
            rows = pl.ds(pl.multiple_of(q * ROWS, ROWS), ROWS)
            sv = ssq[rows, :]
            for lt in range(n_lt):
                cols = slice(lt * LANES, (lt + 1) * LANES)
                nw = nw_ref[:, pl.ds(pl.multiple_of(b * LB + lt * LANES, LANES), LANES)]
                zb[b, rows, cols] = (yb[b, rows, cols] * sv * nw).astype(BF16)
        gcopy(b).start()

    @pl.when(me < n_seq - 1)
    def _():
        halo_send.wait_send()

    all_copies(dg, dg, dgs_sem, dg_sem).wait_send()

    @pl.loop(0, npair)
    def _(i):
        part_copy(i).wait_send()
        all_copies(tc.at[i], hrecv.at[i], s1_sem.at[i], r1_sem.at[i]).wait_send()
        all_copies(hout.at[i], s0r.at[i], s2_sem.at[i], r2_sem.at[i]).wait_send()
        fin_copy(i).wait_send()

    @pl.loop(0, nb)
    def _(b):
        gcopy(b).wait()


def mixer(n_seq, x, doc_start, w_in, conv_w, conv_b, dt_bias, a_log, d_skip, norm_w):
    n_tok, d_model = x.shape
    d_inner = norm_w.shape[0] * norm_w.shape[1]
    n_heads = a_log.shape[0]
    state_dim = (conv_w.shape[1] - d_inner) // 2
    nb = d_inner // LB
    npair = nb // 2
    n_chip = n_seq // 2
    hrows = state_dim // n_chip
    dims = (n_seq, n_tok, d_model, d_inner, n_heads, state_dim)
    vmem = pl.BlockSpec(memory_space=pltpu.VMEM)
    anyspace = pl.BlockSpec(memory_space=pl.ANY)
    dma = pltpu.SemaphoreType.DMA
    scratch = [
        pltpu.VMEM((n_tok + HALO, d_model), BF16),
        pltpu.VMEM((3, LB, d_model), BF16),
        pltpu.VMEM((2 * state_dim + LANES, d_model), BF16),
        pltpu.VMEM((nb, n_tok, LB), BF16),
        pltpu.VMEM((nb, n_tok, LB), BF16),
        pltpu.VMEM((nb, n_tok, LB), F32),
        pltpu.VMEM((n_tok + HALO, LB), F32),
        pltpu.VMEM((n_tok, LB), BF16),
        pltpu.VMEM((nb, state_dim, LB), F32),
        pltpu.VMEM((npair, state_dim, LB), F32),
        pltpu.VMEM((npair, 2, state_dim, LB), F32),
        pltpu.VMEM((npair, n_chip, hrows, LB), F32),
        pltpu.VMEM((npair, n_chip, hrows, LB), F32),
        pltpu.VMEM((npair, n_chip, hrows, LB), F32),
        pltpu.VMEM((npair, n_chip, hrows, LB), F32),
        pltpu.VMEM((npair, 2, state_dim, LB), F32),
        pltpu.VMEM((npair, state_dim, LB), F32),
        pltpu.VMEM((n_tok, 2 * state_dim), BF16),
        pltpu.VMEM((n_tok // CHUNK, state_dim, CHUNK), BF16),
        pltpu.VMEM((n_tok // CHUNK, CHUNK, CHUNK), F32),
        pltpu.VMEM((n_tok, LANES), F32),
        pltpu.VMEM((LANES, n_tok), F32),
        pltpu.VMEM((LANES, n_tok), F32),
        pltpu.VMEM((n_tok, LANES), F32),
        pltpu.VMEM((n_tok, LANES), F32),
        pltpu.VMEM((n_tok, LANES), F32),
        pltpu.VMEM((8, LANES), F32),
        pltpu.VMEM((8, LANES), F32),
        pltpu.VMEM((2, 8, LANES), F32),
        pltpu.VMEM((8, LANES), F32),
        pltpu.VMEM((n_chip, 8, LANES), F32),
        pltpu.VMEM((3, n_tok, LANES), F32),
        pltpu.VMEM((n_tok, LANES), F32),
        pltpu.VMEM((HALO, d_model), BF16),
        dma(()), dma((3,)), dma(()), dma(()), dma(()), dma(()), dma(()), dma(()), dma(()),
        dma((npair,)), dma((npair,)), dma((npair,)), dma((npair,)), dma((npair,)), dma((npair,)), dma((npair,)), dma((npair,)),
        dma((nb,)),
    ]
    return pl.pallas_call(
        functools.partial(mixer_kernel, dims),
        out_shape=jax.ShapeDtypeStruct((n_tok, d_inner), BF16),
        in_specs=[anyspace, vmem, anyspace, vmem, vmem, vmem, vmem, vmem, vmem],
        out_specs=anyspace,
        scratch_shapes=scratch,
        compiler_params=pltpu.CompilerParams(collective_id=0, has_side_effects=True, vmem_limit_bytes=66 * 1000 * 1000),
        name='mixer',
    )(x, doc_start.reshape(n_tok // LANES, LANES), w_in.T, conv_w, conv_b.reshape(1, -1), dt_bias.reshape(1, -1),
      a_log.reshape(1, -1), d_skip.reshape(1, -1), norm_w.reshape(1, -1))


def solution(mesh):
    n_seq = mesh.shape['sp']
    row_spec = P(('dp', 'sp'), None)
    tok_spec = P(('dp', 'sp'))

    def layer_shard(x, doc_start, w_in, conv_w, conv_b, dt_bias, a_log, d_skip, norm_w, w_out):
        g = mixer(n_seq, x, doc_start, w_in, conv_w, conv_b, dt_bias, a_log, d_skip, norm_w)
        return jnp.dot(g, w_out, preferred_element_type=F32).astype(BF16)

    return jax.shard_map(layer_shard, mesh=mesh, in_specs=(row_spec, tok_spec, P(), P(), P(), P(), P(), P(), P(), P()), out_specs=row_spec, check_vma=False)
```

```python
import functools
import math

import jax
import jax.numpy as jnp
from jax import lax
from jax.experimental import pallas as pl
from jax.experimental.pallas import tpu as pltpu
from jax.sharding import PartitionSpec as P

CHUNK = 256
HALF = 128
EPS = 1e-5
LB = 512
LANES = 128
HALO = 16
ROWS = 64
LOG2E = math.log2(math.e)
MESH = pl.DeviceIdType.MESH
F32 = jnp.float32
BF16 = jnp.bfloat16


def dot(a, b):
    return jnp.dot(a, b, preferred_element_type=F32)


def dot_nt(a, b):
    return lax.dot_general(a, b, (((1,), (1,)), ((), ())), preferred_element_type=F32)


def split3(v):
    s1 = v.astype(BF16)
    r1 = v - s1.astype(F32)
    s2 = r1.astype(BF16)
    s3 = (r1 - s2.astype(F32)).astype(BF16)
    return s1, s2, s3


def half_silu(c):
    return c + c * jnp.tanh(c)


def mixer_kernel(dims, x_hbm, ds_ref, w_hbm, wo_hbm, cw_ref, cb_ref, dtb_ref, alog_ref, dsk_ref, nw_ref, o_hbm,
                 xe, wbuf, wbcd, zb, xb, yb, us, us2, sc, mix, cs0, tsend, two, tc, hrecv, hout, s0r, fbuf, soth,
                 bc, bt, gm, a2, apt, ldt, we, ws, arl, prm, dec, dpair, dchip, dg, mk, ssq, hal,
                 xsem, wsem, bsem, hs_sem, hr_sem, dp_sem, dps_sem, dg_sem, dgs_sem,
                 ps_sem, pr_sem, s1_sem, r1_sem, s2_sem, r2_sem, fs_sem, fr_sem, gsem):
    n_seq, n_tok, d_model, d_inner, n_heads, state_dim = dims
    head_dim = d_inner // n_heads
    nb = d_inner // LB
    hb = LB // head_dim
    npair = nb // 2
    n_chip = n_seq // 2
    hrows = state_dim // n_chip
    n_bcd = 2 * state_dim + n_heads
    n_lt = LB // LANES
    n_zfirst = 2

    me = lax.axis_index('sp')
    chip = me // 2
    core = lax.rem(me, 2)
    partner = chip * 2 + (1 - core)

    def dev(i):
        return {'sp': i}

    def wcol(t):
        i2 = t - n_zfirst
        pair = i2 // 2
        own = lax.rem(i2, 2)
        ub = 2 * pair + jnp.where(own == 0, 1 - core, core)
        col = jnp.where(t < n_zfirst, t * LB,
                        jnp.where(t < n_zfirst + nb, d_inner + ub * LB, (t - nb) * LB))
        return pl.multiple_of(col, LB)

    def wcopy(t):
        slot = lax.rem(t, 3)
        return pltpu.make_async_copy(w_hbm.at[pl.ds(wcol(t), LB)], wbuf.at[slot], wsem.at[slot])

    n_steps = 3 * nb

    def wnext(t):
        slot = lax.rem(t, 3)
        pltpu.make_async_copy(w_hbm.at[pl.ds(0, LB)], wbuf.at[slot], wsem.at[slot]).wait()

        @pl.when(t + 2 < 2 * nb)
        def _():
            wcopy(t + 2).start()

        @pl.when(jnp.logical_and(t + 2 >= 2 * nb, t + 2 < n_steps))
        def _():
            slot = lax.rem(t + 2, 3)
            pltpu.make_async_copy(wo_hbm.at[pl.ds(pl.multiple_of((t + 2 - 2 * nb) * LB, LB), LB)], wbuf.at[slot], wsem.at[slot]).start()

    xcopy = pltpu.make_async_copy(x_hbm, xe.at[pl.ds(HALO, n_tok)], xsem)
    xcopy.start()
    wcopy(jnp.int32(0)).start()
    bcopy = pltpu.make_async_copy(w_hbm.at[pl.ds(2 * d_inner, n_bcd)], wbcd.at[pl.ds(0, n_bcd)], bsem)
    bcopy.start()
    wbcd[n_bcd:, :] = jnp.zeros((LANES - n_heads, d_model), BF16)
    wcopy(jnp.int32(1)).start()

    barrier = pltpu.get_barrier_semaphore()
    pl.semaphore_signal(barrier, inc=1, device_id=dev(lax.rem(me + 1, n_seq)), device_id_type=MESH)
    pl.semaphore_signal(barrier, inc=1, device_id=dev(lax.rem(me + n_seq - 1, n_seq)), device_id_type=MESH)

    @pl.loop(1, n_chip)
    def _(r):
        pl.semaphore_signal(barrier, inc=1, device_id=dev(lax.rem(me + 2 * r, n_seq)), device_id_type=MESH)

    ri = lax.broadcasted_iota(jnp.int32, (CHUNK, CHUNK), 0)
    ci = lax.broadcasted_iota(jnp.int32, (CHUNK, CHUNK), 1)
    tri = (ri >= ci).astype(F32).astype(BF16)
    eye = (ri == ci).astype(F32).astype(BF16)
    n_chunks = n_tok // CHUNK
    per = CHUNK // LANES
    seg_cols, seg_rows, ds_cols = [], [], []
    for c in range(n_chunks):
        row = jnp.concatenate([ds_ref[per * c + q:per * c + q + 1, :] for q in range(per)], axis=1).astype(F32)
        row = jnp.broadcast_to(row, (8, CHUNK)).astype(BF16)
        ds_cols.append(jnp.broadcast_to(dot_nt(eye, row)[:, 0:1], (CHUNK, LANES)))
        seg_cols.append(jnp.broadcast_to(dot_nt(tri, row)[:, 0:1], (CHUNK, LANES)))
        seg_rows.append(dot_nt(row, tri)[0:1, :])
    keep = 1.0 - jnp.concatenate(ds_cols, axis=0)
    tok = lax.broadcasted_iota(jnp.int32, (n_tok, LANES), 0)
    m1 = keep
    k1 = jnp.where(tok >= 1, pltpu.roll(keep, 1, 0), 1.0)
    k2 = jnp.where(tok >= 2, pltpu.roll(keep, 2, 0), 1.0)
    mk[0] = m1
    mk[1] = m1 * k1
    mk[2] = m1 * k1 * k2

    xcopy.wait()
    hrow = lax.broadcasted_iota(jnp.int32, (HALO, LANES), 0)
    k_last = jnp.broadcast_to(mk[0, n_tok - 8:n_tok, :][7:8, :], (HALO, LANES))
    k_last2 = jnp.broadcast_to(mk[1, n_tok - 8:n_tok, :][7:8, :], (HALO, LANES))
    hmask = jnp.where(hrow == HALO - 1, 1.0, jnp.where(hrow == HALO - 2, k_last, jnp.where(hrow == HALO - 3, k_last2, 0.0)))
    for q in range(d_model // LANES):
        hal[:, q * LANES:(q + 1) * LANES] = (xe[n_tok:n_tok + HALO, q * LANES:(q + 1) * LANES].astype(F32) * hmask).astype(BF16)

    def zblock(t, zi):
        wnext(t)
        slot = lax.rem(t, 3)
        for q in range(n_tok // CHUNK):
            zb[zi, q * CHUNK:(q + 1) * CHUNK] = dot_nt(xe[HALO + q * CHUNK:HALO + (q + 1) * CHUNK], wbuf[slot]).astype(BF16)

    pl.semaphore_wait(barrier, n_chip + 1)
    halo_send = pltpu.make_async_remote_copy(
        src_ref=hal, dst_ref=xe.at[pl.ds(0, HALO)], send_sem=hs_sem, recv_sem=hr_sem,
        device_id=dev(lax.rem(me + 1, n_seq)), device_id_type=MESH)

    @pl.when(me < n_seq - 1)
    def _():
        halo_send.start()

    @pl.when(me == 0)
    def _():
        xe[0:HALO, :] = jnp.zeros((HALO, d_model), BF16)

    @pl.loop(0, n_zfirst)
    def _(t):
        zblock(t, t)

    @pl.when(me > 0)
    def _():
        halo_send.wait_recv()

    bcopy.wait()
    mrow = (n_tok + HALO) // 2
    lane = lax.broadcasted_iota(jnp.int32, (1, LANES), 1)
    for q in range(2):
        us2[q * mrow:(q + 1) * mrow, 0:2 * state_dim + LANES] = dot_nt(xe[q * mrow:(q + 1) * mrow], wbcd[...]).astype(BF16).astype(F32)

    def udot(slot, u_ref, q):
        u_ref[q * mrow:(q + 1) * mrow, :] = dot_nt(xe[q * mrow:(q + 1) * mrow], wbuf[slot]).astype(BF16).astype(F32)

    t_u = n_zfirst
    wnext(jnp.int32(t_u))
    udot(t_u % 3, us, 0)
    udot(t_u % 3, us, 1)

    def conv(u_ref, r0, lt, wl):
        cols = slice(lt * LANES, (lt + 1) * LANES)
        ext = u_ref[pl.ds(pl.multiple_of(r0 + HALO - 8, 8), ROWS + 8), cols]
        wl = pl.multiple_of(wl, LANES)
        cw = cw_ref[:, pl.ds(wl, LANES)] * 0.5
        v = cb_ref[pl.ds(wl // LANES, 1), :] * 0.5 + cw[0:1] * ext[8:8 + ROWS]
        for k in range(1, 4):
            v = v + cw[k:k + 1] * (mk[k - 1, pl.ds(r0, ROWS), :] * ext[8 - k:8 - k + ROWS])
        return half_silu(v)

    @pl.loop(0, n_tok // ROWS, unroll=True)
    def _(q):
        r0 = pl.multiple_of(q * ROWS, ROWS)
        for lt in range(2 * state_dim // LANES):
            bc[pl.ds(r0, ROWS), lt * LANES:(lt + 1) * LANES] = conv(us2, r0, lt, d_inner + lt * LANES).astype(BF16)

    prm[...] = jnp.zeros((8, LANES), F32)
    prm[0:1, 0:n_heads] = dtb_ref[...]
    prm[1:2, 0:n_heads] = alog_ref[...]
    prm[2:3, 0:n_heads] = dsk_ref[...]
    pv = prm[...]
    head_ok = lane < n_heads
    neg_a = jnp.where(head_ok, -jnp.exp(pv[1:2]) , 0.0)
    e_rows = []
    for c in range(n_chunks):
        rows = slice(c * CHUNK, (c + 1) * CHUNK)
        raw = jnp.where(head_ok, us2[HALO + c * CHUNK:HALO + (c + 1) * CHUNK, 2 * state_dim:2 * state_dim + LANES], 0.0) + pv[0:1]
        dt = jnp.maximum(raw, 0.0) + jnp.log1p(jnp.exp(-jnp.abs(raw)))
        s1, s2, s3 = split3(neg_a * dt * LOG2E)
        acum = dot(tri, s3) + dot(tri, s2) + dot(tri, s1)
        a2[rows, :] = acum
        a_t = jnp.transpose(acum)
        ld_t = jnp.transpose(jnp.log2(dt))
        ldt[:, rows] = ld_t
        apt[:, rows] = a_t - ld_t
        seg = seg_cols[c]
        last = acum[CHUNK - 1:CHUNK, :]
        seg_last = seg[CHUNK - 1:CHUNK, :]
        ws[rows, :] = jnp.where(seg == 0.0, jnp.exp2(acum), 0.0)
        we[rows, :] = jnp.where(seg == seg_last, jnp.exp2(last - acum) * dt, 0.0)
        e_rows.append(jnp.where(seg_last == 0.0, jnp.exp2(last), 0.0))
        b_c = bc[rows, 0:state_dim]
        c_c = bc[rows, state_dim:2 * state_dim]
        b_t = jnp.transpose(b_c.astype(F32)).astype(BF16)
        bt[c] = b_t
        scores = dot(c_c, b_t)
        same = jnp.concatenate([seg] * per, axis=1) == seg_rows[c]
        gm[c] = jnp.where(jnp.logical_and(ri >= ci, same), scores, 0.0)
    d_own = e_rows[0] * e_rows[1]
    dec[0:1, :] = e_rows[0]
    dec[1:2, :] = e_rows[1]
    dpair[core] = jnp.broadcast_to(d_own, (8, LANES))

    pair_send = pltpu.make_async_remote_copy(
        src_ref=dpair.at[core], dst_ref=dpair.at[core], send_sem=dps_sem, recv_sem=dp_sem,
        device_id=dev(partner), device_id_type=MESH)
    pair_send.start()

    def send_decays():
        pair_send.wait()
        dchip[...] = dpair[0] * dpair[1]
        dg[chip] = dpair[0] * dpair[1]
        dec[2:3, :] = dpair[0][0:1]
        dec[3:4, :] = dpair[1][0:1]

        @pl.loop(1, n_chip)
        def _(r):
            q = lax.rem(chip + r, n_chip)
            pltpu.make_async_remote_copy(
                src_ref=dchip, dst_ref=dg.at[chip], send_sem=dgs_sem, recv_sem=dg_sem,
                device_id=dev(2 * q + core), device_id_type=MESH).start()

    def expand(v, b):
        n = v.shape[0]
        r = pltpu.roll(v, lax.rem(2 * LANES - hb * b, LANES), 1)
        low = lax.broadcasted_iota(jnp.int32, (n, LANES), 1) < head_dim
        out = []
        for p in range(n_lt):
            out.append(jnp.where(low, jnp.broadcast_to(r[:, 2 * p:2 * p + 1], (n, LANES)),
                                 jnp.broadcast_to(r[:, 2 * p + 1:2 * p + 2], (n, LANES))))
        return jnp.concatenate(out, axis=1)

    def roll_to(dst, src, b):
        sh = lax.rem(2 * LANES - hb * b, LANES)
        for q in range(n_tok // LANES):
            dst[q * LANES:(q + 1) * LANES, :] = pltpu.roll(src[q * LANES:(q + 1) * LANES, :], sh, 1)

    low_r = lax.broadcasted_iota(jnp.int32, (ROWS, LANES), 1) < head_dim

    def head_cols(r0, lt):
        wv = arl[pl.ds(r0, ROWS), :]
        return jnp.where(low_r, jnp.broadcast_to(wv[:, 2 * lt:2 * lt + 1], (ROWS, LANES)),
                         jnp.broadcast_to(wv[:, 2 * lt + 1:2 * lt + 2], (ROWS, LANES)))

    def ublock(t_next, u_next, u_ref, b, t_ref):
        wnext(t_next)
        slot = lax.rem(t_next, 3)
        roll_to(arl, we, b)
        for half in range(2):
            udot(slot, u_next, half)

            @pl.loop(0, n_tok // ROWS // 2, unroll=True)
            def _(q):
                r0 = pl.multiple_of(half * (n_tok // 2) + q * ROWS, ROWS)
                for lt in range(n_lt):
                    cols = slice(lt * LANES, (lt + 1) * LANES)
                    xs = conv(u_ref, r0, lt, b * LB + lt * LANES).astype(BF16)
                    xb[b, pl.ds(r0, ROWS), cols] = xs
                    sc[pl.ds(r0, ROWS), cols] = (xs.astype(F32) * head_cols(r0, lt)).astype(BF16)

        ex = expand(dec[...], b)
        st0 = dot(bt[0], sc[0:CHUNK])
        cs0[b] = st0
        t_ref[...] = ex[1:2] * st0 + dot(bt[1], sc[CHUNK:2 * CHUNK])

    def part_copy(i):
        return pltpu.make_async_remote_copy(
            src_ref=tsend.at[i], dst_ref=two.at[i, core], send_sem=ps_sem.at[i], recv_sem=pr_sem.at[i],
            device_id=dev(partner), device_id_type=MESH)

    def home_copy(i, q):
        return pltpu.make_async_remote_copy(
            src_ref=tc.at[i, q], dst_ref=hrecv.at[i, chip], send_sem=s1_sem.at[i], recv_sem=r1_sem.at[i],
            device_id=dev(2 * q + core), device_id_type=MESH)

    def back_copy(i, q):
        return pltpu.make_async_remote_copy(
            src_ref=hout.at[i, q], dst_ref=s0r.at[i, chip], send_sem=s2_sem.at[i], recv_sem=r2_sem.at[i],
            device_id=dev(2 * q + core), device_id_type=MESH)

    def all_copies(src, dst, send_sem, recv_sem):
        return pltpu.make_async_remote_copy(
            src_ref=src.at[pl.ds(0, n_chip - 1)], dst_ref=dst.at[pl.ds(0, n_chip - 1)], send_sem=send_sem, recv_sem=recv_sem,
            device_id=dev(partner), device_id_type=MESH)

    def fin_copy(i):
        return pltpu.make_async_remote_copy(
            src_ref=fbuf.at[i, 1 - core], dst_ref=soth.at[i], send_sem=fs_sem.at[i], recv_sem=fr_sem.at[i],
            device_id=dev(partner), device_id_type=MESH)

    def send_home(i, b):
        part_copy(i).wait_recv()
        ex = expand(dec[...], b)
        for q in range(n_chip):
            rows = slice(q * hrows, (q + 1) * hrows)
            tc[i, q] = ex[3:4] * two[i, 0, rows] + two[i, 1, rows]
        hrecv[i, chip] = tc[i, chip]

        @pl.loop(1, n_chip)
        def _(r):
            home_copy(i, lax.rem(chip + r, n_chip)).start()

    def home(i):
        b = 2 * i + core
        all_copies(tc.at[i], hrecv.at[i], s1_sem.at[i], r1_sem.at[i]).wait_recv()
        run = jnp.zeros((hrows, LB), F32)
        for q in range(n_chip):
            hout[i, q] = run
            run = expand(dg[q], b)[0:1] * run + hrecv[i, q]
        s0r[i, chip] = hout[i, chip]

        @pl.loop(1, n_chip)
        def _(r):
            back_copy(i, lax.rem(chip + r, n_chip)).start()

    def finish(i):
        b = 2 * i + core
        all_copies(hout.at[i], s0r.at[i], s2_sem.at[i], r2_sem.at[i]).wait_recv()
        ex = expand(dec[...], b)
        for q in range(n_chip):
            rows = slice(q * hrows, (q + 1) * hrows)
            fbuf[i, 0, rows] = s0r[i, q]
            fbuf[i, 1, rows] = ex[2:3] * s0r[i, q] + two[i, 0, rows]
        fin_copy(i).start()

    @pl.loop(0, npair)
    def _(i):
        t = n_zfirst + 2 * i
        ublock(t + 1, us2, us, 2 * i + 1 - core, tsend.at[i])
        part_copy(i).start()

        @pl.when(i == 0)
        def _():
            send_decays()

        ublock(t + 2, us, us2, 2 * i + core, two.at[i, core])
        send_home(i, 2 * i + core)

        @pl.when(i == 0)
        def _():
            all_copies(dg, dg, dgs_sem, dg_sem).wait_recv()

        @pl.when(i >= 1)
        def _():
            home(i - 1)

        @pl.when(i >= 2)
        def _():
            finish(i - 2)

    zb[n_zfirst] = us[HALO:HALO + n_tok, :].astype(BF16)

    low_b = (lax.broadcasted_iota(jnp.int32, (CHUNK, LANES), 1) < head_dim).astype(F32).astype(BF16)
    high_b = (lax.broadcasted_iota(jnp.int32, (CHUNK, LANES), 1) >= head_dim).astype(F32).astype(BF16)

    sub = 32

    def intra(b):
        heads = pl.ds(pl.multiple_of(b * hb, hb), hb)
        dsk = expand(prm[...], b)[2:3]
        for c in range(n_chunks):
            r0 = c * CHUNK
            ap8 = apt[heads, r0:r0 + CHUNK]
            ld8 = ldt[heads, r0:r0 + CHUNK]
            for p in range(n_lt):
                cols = slice(p * LANES, (p + 1) * LANES)
                k = p % 4
                for hh in range(2):
                    h = 2 * p + hh
                    aj0, aj1 = ap8[h:h + 1, :HALF], ap8[h:h + 1, HALF:]
                    ld0, ld1 = ld8[h:h + 1, :HALF], ld8[h:h + 1, HALF:]
                    base = CHUNK + hh * CHUNK
                    for q in range(HALF // sub):
                        rr = slice(q * sub, (q + 1) * sub)
                        g0 = slice(q * sub, (q + 1) * sub)
                        g1 = slice(HALF + q * sub, HALF + (q + 1) * sub)
                        ai0 = jnp.broadcast_to(arl[r0 + q * sub:r0 + (q + 1) * sub, h:h + 1], (sub, HALF))
                        ai1 = jnp.broadcast_to(arl[r0 + HALF + q * sub:r0 + HALF + (q + 1) * sub, h:h + 1], (sub, HALF))
                        mix[k, rr, hh * HALF:(hh + 1) * HALF] = (jnp.exp2(jnp.minimum(ai0 - aj0, ld0)) * gm[c, g0, 0:HALF]).astype(BF16)
                        mix[k, rr, base:base + HALF] = (jnp.exp2(ai1 - aj0) * gm[c, g1, 0:HALF]).astype(BF16)
                        mix[k, rr, base + HALF:base + CHUNK] = (jnp.exp2(jnp.minimum(ai1 - aj1, ld1)) * gm[c, g1, HALF:CHUNK]).astype(BF16)
                xp = xb[b, r0:r0 + CHUNK, cols]
                xa, xh = xp * low_b, xp * high_b
                y0 = dot(mix[k, :, 0:CHUNK], jnp.concatenate([xa[:HALF], xh[:HALF]], axis=0))
                y1 = dot(mix[k, :, CHUNK:3 * CHUNK], jnp.concatenate([xa, xh], axis=0))
                yb[b, r0:r0 + HALF, cols] = y0 + dsk[:, cols] * xp[:HALF].astype(F32)
                yb[b, r0 + HALF:r0 + CHUNK, cols] = y1 + dsk[:, cols] * xp[HALF:].astype(F32)

    n_with = nb - n_zfirst - 1

    @pl.loop(0, n_with)
    def _(m):
        t = m + n_zfirst + 1 + nb
        wnext(t)
        slot = lax.rem(t, 3)
        roll_to(arl, a2, m)
        for q in range(n_tok // CHUNK):
            zb[m + n_zfirst + 1, q * CHUNK:(q + 1) * CHUNK] = dot_nt(xe[HALO + q * CHUNK:HALO + (q + 1) * CHUNK], wbuf[slot]).astype(BF16)
        intra(m)

        @pl.when(m == 1)
        def _():
            home(npair - 1)
            finish(npair - 2)

        @pl.when(m == n_with - 1)
        def _():
            finish(npair - 1)

    @pl.loop(n_with, nb)
    def _(m):
        roll_to(arl, a2, m)
        intra(m)

    ssq[...] = jnp.zeros((n_tok, LANES), F32)

    def close(b, s_ref):
        ex = expand(dec[...], b)
        roll_to(arl, ws, b)
        s_in = s_ref[...]
        us[0:CHUNK, :] = dot(bc[0:CHUNK, state_dim:2 * state_dim], s_in.astype(BF16))
        s_mid = ex[0:1] * s_in + cs0[b]
        us[CHUNK:2 * CHUNK, :] = dot(bc[CHUNK:2 * CHUNK, state_dim:2 * state_dim], s_mid.astype(BF16))

        @pl.loop(0, n_tok // ROWS, unroll=True)
        def _(q):
            rows = pl.ds(pl.multiple_of(q * ROWS, ROWS), ROWS)
            acc = ssq[rows, :]
            for lt in range(n_lt):
                cols = slice(lt * LANES, (lt + 1) * LANES)
                y = yb[b, rows, cols] + head_cols(q * ROWS, lt) * us[rows, cols]
                gated = y * half_silu(zb[b, rows, cols].astype(F32) * 0.5)
                yb[b, rows, cols] = gated
                acc = acc + gated * gated
            ssq[rows, :] = acc

    @pl.loop(0, npair)
    def _(i):
        close(2 * i + core, fbuf.at[i, core])
        fin_copy(i).wait_recv()
        close(2 * i + 1 - core, soth.at[i])

    scale = lax.rsqrt(jnp.sum(ssq[...], axis=1, keepdims=True) * (1.0 / d_inner) + EPS)
    ssq[...] = jnp.broadcast_to(scale, (n_tok, LANES))

    n_out = d_model // LB

    def normalize(b):
        @pl.loop(0, n_tok // ROWS, unroll=True)
        def _(q):
            rows = pl.ds(pl.multiple_of(q * ROWS, ROWS), ROWS)
            sv = ssq[rows, :]
            for lt in range(n_lt):
                cols = slice(lt * LANES, (lt + 1) * LANES)
                nw = nw_ref[:, pl.ds(pl.multiple_of(b * LB + lt * LANES, LANES), LANES)]
                zb[b, rows, cols] = (yb[b, rows, cols] * sv * nw).astype(BF16)

    @pl.loop(0, n_out)
    def _(b):
        normalize(b)

    def project(b, first, last):
        wnext(b + 2 * nb)
        slot = lax.rem(b + 2 * nb, 3)
        for n in range(n_out):
            part = dot(zb[b], wbuf[slot, :, n * LB:(n + 1) * LB])
            if not first:
                part = yb[n] + part
            if last:
                xb[n] = part.astype(BF16)
            else:
                yb[n] = part

    def ocopy(n):
        return pltpu.make_async_copy(xb.at[n], o_hbm.at[:, n * LB:(n + 1) * LB], gsem.at[n])

    project(jnp.int32(0), True, False)

    @pl.loop(1, nb - 1)
    def _(b):
        @pl.when(b >= n_out - 1)
        def _():
            normalize(b + 1)
        project(b, False, False)

    project(jnp.int32(nb - 1), False, True)
    for n in range(n_out):
        ocopy(n).start()

    @pl.when(me < n_seq - 1)
    def _():
        halo_send.wait_send()

    all_copies(dg, dg, dgs_sem, dg_sem).wait_send()

    @pl.loop(0, npair)
    def _(i):
        part_copy(i).wait_send()
        all_copies(tc.at[i], hrecv.at[i], s1_sem.at[i], r1_sem.at[i]).wait_send()
        all_copies(hout.at[i], s0r.at[i], s2_sem.at[i], r2_sem.at[i]).wait_send()
        fin_copy(i).wait_send()

    for n in range(n_out):
        ocopy(n).wait()


def mixer(n_seq, x, doc_start, w_in, conv_w, conv_b, dt_bias, a_log, d_skip, norm_w, w_out):
    n_tok, d_model = x.shape
    d_inner = norm_w.shape[0] * norm_w.shape[1]
    n_heads = a_log.shape[0]
    state_dim = (conv_w.shape[1] - d_inner) // 2
    nb = d_inner // LB
    npair = nb // 2
    n_chip = n_seq // 2
    hrows = state_dim // n_chip
    dims = (n_seq, n_tok, d_model, d_inner, n_heads, state_dim)
    vmem = pl.BlockSpec(memory_space=pltpu.VMEM)
    anyspace = pl.BlockSpec(memory_space=pl.ANY)
    dma = pltpu.SemaphoreType.DMA
    scratch = [
        pltpu.VMEM((n_tok + HALO, d_model), BF16),
        pltpu.VMEM((3, LB, d_model), BF16),
        pltpu.VMEM((2 * state_dim + LANES, d_model), BF16),
        pltpu.VMEM((nb, n_tok, LB), BF16),
        pltpu.VMEM((nb, n_tok, LB), BF16),
        pltpu.VMEM((nb, n_tok, LB), F32),
        pltpu.VMEM((n_tok + HALO, LB), F32),
        pltpu.VMEM((n_tok + HALO, LB), F32),
        pltpu.VMEM((n_tok, LB), BF16),
        pltpu.VMEM((4, HALF, 3 * CHUNK), BF16),
        pltpu.VMEM((nb, state_dim, LB), F32),
        pltpu.VMEM((npair, state_dim, LB), F32),
        pltpu.VMEM((npair, 2, state_dim, LB), F32),
        pltpu.VMEM((npair, n_chip, hrows, LB), F32),
        pltpu.VMEM((npair, n_chip, hrows, LB), F32),
        pltpu.VMEM((npair, n_chip, hrows, LB), F32),
        pltpu.VMEM((npair, n_chip, hrows, LB), F32),
        pltpu.VMEM((npair, 2, state_dim, LB), F32),
        pltpu.VMEM((npair, state_dim, LB), F32),
        pltpu.VMEM((n_tok, 2 * state_dim), BF16),
        pltpu.VMEM((n_tok // CHUNK, state_dim, CHUNK), BF16),
        pltpu.VMEM((n_tok // CHUNK, CHUNK, CHUNK), F32),
        pltpu.VMEM((n_tok, LANES), F32),
        pltpu.VMEM((LANES, n_tok), F32),
        pltpu.VMEM((LANES, n_tok), F32),
        pltpu.VMEM((n_tok, LANES), F32),
        pltpu.VMEM((n_tok, LANES), F32),
        pltpu.VMEM((n_tok, LANES), F32),
        pltpu.VMEM((8, LANES), F32),
        pltpu.VMEM((8, LANES), F32),
        pltpu.VMEM((2, 8, LANES), F32),
        pltpu.VMEM((8, LANES), F32),
        pltpu.VMEM((n_chip, 8, LANES), F32),
        pltpu.VMEM((3, n_tok, LANES), F32),
        pltpu.VMEM((n_tok, LANES), F32),
        pltpu.VMEM((HALO, d_model), BF16),
        dma(()), dma((3,)), dma(()), dma(()), dma(()), dma(()), dma(()), dma(()), dma(()),
        dma((npair,)), dma((npair,)), dma((npair,)), dma((npair,)), dma((npair,)), dma((npair,)), dma((npair,)), dma((npair,)),
        dma((d_model // LB,)),
    ]
    return pl.pallas_call(
        functools.partial(mixer_kernel, dims),
        out_shape=jax.ShapeDtypeStruct((n_tok, d_model), BF16),
        in_specs=[anyspace, vmem, anyspace, anyspace, vmem, vmem, vmem, vmem, vmem, vmem],
        out_specs=anyspace,
        scratch_shapes=scratch,
        compiler_params=pltpu.CompilerParams(collective_id=0, has_side_effects=True, vmem_limit_bytes=66 * 1000 * 1000),
        name='mixer',
    )(x, doc_start.reshape(n_tok // LANES, LANES), w_in.T, w_out, conv_w, conv_b.reshape(-1, LANES), dt_bias.reshape(1, -1),
      a_log.reshape(1, -1), d_skip.reshape(1, -1), norm_w.reshape(1, -1))


def solution(mesh):
    n_seq = mesh.shape['sp']
    row_spec = P(('dp', 'sp'), None)
    tok_spec = P(('dp', 'sp'))

    def layer_shard(x, doc_start, w_in, conv_w, conv_b, dt_bias, a_log, d_skip, norm_w, w_out):
        return mixer(n_seq, x, doc_start, w_in, conv_w, conv_b, dt_bias, a_log, d_skip, norm_w, w_out)

    return jax.shard_map(layer_shard, mesh=mesh, in_specs=(row_spec, tok_spec, P(), P(), P(), P(), P(), P(), P(), P()), out_specs=row_spec, check_vma=False)
```

```python
import functools
import math

import jax
import jax.numpy as jnp
from jax import lax
from jax.experimental import pallas as pl
from jax.experimental.pallas import tpu as pltpu
from jax.sharding import PartitionSpec as P

CHUNK = 256
HALF = 128
EPS = 1e-5
LB = 512
LANES = 128
HALO = 16
ROWS = 64
LOG2E = math.log2(math.e)
MESH = pl.DeviceIdType.MESH
F32 = jnp.float32
BF16 = jnp.bfloat16


def dot(a, b):
    return jnp.dot(a, b, preferred_element_type=F32)


def dot_nt(a, b):
    return lax.dot_general(a, b, (((1,), (1,)), ((), ())), preferred_element_type=F32)


def split3(v):
    s1 = v.astype(BF16)
    r1 = v - s1.astype(F32)
    s2 = r1.astype(BF16)
    s3 = (r1 - s2.astype(F32)).astype(BF16)
    return s1, s2, s3


def half_silu(c):
    return c + c * jnp.tanh(c)


def mixer_kernel(dims, x_hbm, ds_ref, w_hbm, wo_hbm, cw_ref, cb_ref, dtb_ref, alog_ref, dsk_ref, nw_ref, o_hbm,
                 xe, wbuf, wbcd, zb, xb, yb, us, us2, yst, sc, mix, cs0, tsend, two, tc, hrecv, hout, s0r, fbuf, soth,
                 bc, bt, gm, a2, apt, ldt, we, ws, arl, prm, dec, dpair, dchip, dg, mk, ssq, hal,
                 xsem, wsem, bsem, hs_sem, hr_sem, dp_sem, dps_sem, dg_sem, dgs_sem,
                 ps_sem, pr_sem, s1_sem, r1_sem, s2_sem, r2_sem, fs_sem, fr_sem, gsem):
    n_seq, n_tok, d_model, d_inner, n_heads, state_dim = dims
    head_dim = d_inner // n_heads
    nb = d_inner // LB
    hb = LB // head_dim
    npair = nb // 2
    n_chip = n_seq // 2
    hrows = state_dim // n_chip
    n_bcd = 2 * state_dim + n_heads
    n_lt = LB // LANES
    n_zfirst = 2
    t_z = n_zfirst + nb
    n_zmid = npair - 2
    n_zlast = npair - 1

    me = lax.axis_index('sp')
    chip = me // 2
    core = lax.rem(me, 2)
    partner = chip * 2 + (1 - core)

    def dev(i):
        return {'sp': i}

    def wcol(t):
        i2 = t - n_zfirst
        pair = i2 // 2
        own = lax.rem(i2, 2)
        ub = 2 * pair + jnp.where(own == 0, 1 - core, core)
        zi = jnp.where(t <= t_z, n_zfirst, jnp.where(t <= t_z + n_zmid, n_zfirst + 2 * (t - t_z), n_zfirst + 1 + 2 * (t - t_z - n_zmid - 1)))
        col = jnp.where(t < n_zfirst, t * LB,
                        jnp.where(t < n_zfirst + nb, d_inner + ub * LB, zi * LB))
        return pl.multiple_of(col, LB)

    def wcopy(t):
        slot = lax.rem(t, 3)
        return pltpu.make_async_copy(w_hbm.at[pl.ds(wcol(t), LB)], wbuf.at[slot], wsem.at[slot])

    n_steps = 3 * nb

    def wnext(t):
        slot = lax.rem(t, 3)
        pltpu.make_async_copy(w_hbm.at[pl.ds(0, LB)], wbuf.at[slot], wsem.at[slot]).wait()

        @pl.when(t + 2 < 2 * nb)
        def _():
            wcopy(t + 2).start()

        @pl.when(jnp.logical_and(t + 2 >= 2 * nb, t + 2 < n_steps))
        def _():
            slot = lax.rem(t + 2, 3)
            pltpu.make_async_copy(wo_hbm.at[pl.ds(pl.multiple_of((t + 2 - 2 * nb) * LB, LB), LB)], wbuf.at[slot], wsem.at[slot]).start()

    xcopy = pltpu.make_async_copy(x_hbm, xe.at[pl.ds(HALO, n_tok)], xsem)
    xcopy.start()
    wcopy(jnp.int32(0)).start()
    bcopy = pltpu.make_async_copy(w_hbm.at[pl.ds(2 * d_inner, n_bcd)], wbcd.at[pl.ds(0, n_bcd)], bsem)
    bcopy.start()
    wbcd[n_bcd:, :] = jnp.zeros((LANES - n_heads, d_model), BF16)
    wcopy(jnp.int32(1)).start()

    barrier = pltpu.get_barrier_semaphore()
    pl.semaphore_signal(barrier, inc=1, device_id=dev(lax.rem(me + 1, n_seq)), device_id_type=MESH)
    pl.semaphore_signal(barrier, inc=1, device_id=dev(lax.rem(me + n_seq - 1, n_seq)), device_id_type=MESH)

    @pl.loop(1, n_chip)
    def _(r):
        pl.semaphore_signal(barrier, inc=1, device_id=dev(lax.rem(me + 2 * r, n_seq)), device_id_type=MESH)

    ri = lax.broadcasted_iota(jnp.int32, (CHUNK, CHUNK), 0)
    ci = lax.broadcasted_iota(jnp.int32, (CHUNK, CHUNK), 1)
    tri = (ri >= ci).astype(F32).astype(BF16)
    eye = (ri == ci).astype(F32).astype(BF16)
    n_chunks = n_tok // CHUNK
    per = CHUNK // LANES
    seg_cols, seg_rows, ds_cols = [], [], []
    for c in range(n_chunks):
        row = jnp.concatenate([ds_ref[per * c + q:per * c + q + 1, :] for q in range(per)], axis=1).astype(F32)
        row = jnp.broadcast_to(row, (8, CHUNK)).astype(BF16)
        ds_cols.append(jnp.broadcast_to(dot_nt(eye, row)[:, 0:1], (CHUNK, LANES)))
        seg_cols.append(jnp.broadcast_to(dot_nt(tri, row)[:, 0:1], (CHUNK, LANES)))
        seg_rows.append(dot_nt(row, tri)[0:1, :])
    keep = 1.0 - jnp.concatenate(ds_cols, axis=0)
    tok = lax.broadcasted_iota(jnp.int32, (n_tok, LANES), 0)
    m1 = keep
    k1 = jnp.where(tok >= 1, pltpu.roll(keep, 1, 0), 1.0)
    k2 = jnp.where(tok >= 2, pltpu.roll(keep, 2, 0), 1.0)
    mk[0] = m1
    mk[1] = m1 * k1
    mk[2] = m1 * k1 * k2

    xcopy.wait()
    hrow = lax.broadcasted_iota(jnp.int32, (HALO, LANES), 0)
    k_last = jnp.broadcast_to(mk[0, n_tok - 8:n_tok, :][7:8, :], (HALO, LANES))
    k_last2 = jnp.broadcast_to(mk[1, n_tok - 8:n_tok, :][7:8, :], (HALO, LANES))
    hmask = jnp.where(hrow == HALO - 1, 1.0, jnp.where(hrow == HALO - 2, k_last, jnp.where(hrow == HALO - 3, k_last2, 0.0)))
    for q in range(d_model // LANES):
        hal[:, q * LANES:(q + 1) * LANES] = (xe[n_tok:n_tok + HALO, q * LANES:(q + 1) * LANES].astype(F32) * hmask).astype(BF16)

    def zblock(t, zi):
        wnext(t)
        slot = lax.rem(t, 3)
        zb[zi] = dot_nt(xe[HALO:HALO + n_tok], wbuf[slot]).astype(BF16)

    pl.semaphore_wait(barrier, n_chip + 1)
    halo_send = pltpu.make_async_remote_copy(
        src_ref=hal, dst_ref=xe.at[pl.ds(0, HALO)], send_sem=hs_sem, recv_sem=hr_sem,
        device_id=dev(lax.rem(me + 1, n_seq)), device_id_type=MESH)

    @pl.when(me < n_seq - 1)
    def _():
        halo_send.start()

    @pl.when(me == 0)
    def _():
        xe[0:HALO, :] = jnp.zeros((HALO, d_model), BF16)

    @pl.loop(0, n_zfirst)
    def _(t):
        zblock(t, t)

    @pl.when(me > 0)
    def _():
        halo_send.wait_recv()

    bcopy.wait()
    lane = lax.broadcasted_iota(jnp.int32, (1, LANES), 1)
    p_bcd = dot_nt(xe[...], wbcd[...]).astype(BF16).astype(F32)
    for lt in range(2 * state_dim // LANES + 1):
        us2[lt] = p_bcd[:, lt * LANES:(lt + 1) * LANES]

    def udot(slot, u_ref):
        p_u = dot_nt(xe[...], wbuf[slot]).astype(BF16).astype(F32)
        for lt in range(n_lt):
            u_ref[lt] = p_u[:, lt * LANES:(lt + 1) * LANES]

    t_u = n_zfirst
    wnext(jnp.int32(t_u))
    udot(t_u % 3, us)

    def conv(u_ref, r0, lt, wl):
        wl = pl.multiple_of(wl, LANES)
        cw = cw_ref[:, pl.ds(wl, LANES)] * 0.5
        v = cb_ref[pl.ds(wl // LANES, 1), :] * 0.5 + cw[0:1] * u_ref[lt, pl.ds(r0 + HALO, ROWS), :]
        for k in range(1, 4):
            v = v + cw[k:k + 1] * (mk[k - 1, pl.ds(r0, ROWS), :] * u_ref[lt, pl.ds(r0 + HALO - k, ROWS), :])
        return half_silu(v)

    for r0 in range(0, n_tok, ROWS):
        for lt in range(2 * state_dim // LANES):
            bc[r0:r0 + ROWS, lt * LANES:(lt + 1) * LANES] = conv(us2, r0, lt, d_inner + lt * LANES).astype(BF16)

    prm[...] = jnp.zeros((8, LANES), F32)
    prm[0:1, 0:n_heads] = dtb_ref[...]
    prm[1:2, 0:n_heads] = alog_ref[...]
    prm[2:3, 0:n_heads] = dsk_ref[...]
    pv = prm[...]
    head_ok = lane < n_heads
    neg_a = jnp.where(head_ok, -jnp.exp(pv[1:2]) , 0.0)
    e_rows = []
    for c in range(n_chunks):
        rows = slice(c * CHUNK, (c + 1) * CHUNK)
        raw = jnp.where(head_ok, us2[2 * state_dim // LANES, HALO + c * CHUNK:HALO + (c + 1) * CHUNK, :], 0.0) + pv[0:1]
        dt = jnp.maximum(raw, 0.0) + jnp.log1p(jnp.exp(-jnp.abs(raw)))
        s1, s2, s3 = split3(neg_a * dt * LOG2E)
        acum = dot(tri, s3) + dot(tri, s2) + dot(tri, s1)
        a2[rows, :] = acum
        a_t = jnp.transpose(acum)
        ld_t = jnp.transpose(jnp.log2(dt))
        ldt[:, rows] = ld_t
        apt[:, rows] = a_t - ld_t
        seg = seg_cols[c]
        last = acum[CHUNK - 1:CHUNK, :]
        seg_last = seg[CHUNK - 1:CHUNK, :]
        ws[rows, :] = jnp.where(seg == 0.0, jnp.exp2(acum), 0.0)
        we[rows, :] = jnp.where(seg == seg_last, jnp.exp2(last - acum) * dt, 0.0)
        e_rows.append(jnp.where(seg_last == 0.0, jnp.exp2(last), 0.0))
        b_c = bc[rows, 0:state_dim]
        c_c = bc[rows, state_dim:2 * state_dim]
        b_t = jnp.transpose(b_c.astype(F32)).astype(BF16)
        bt[c] = b_t
        scores = dot(c_c, b_t)
        same = jnp.concatenate([seg] * per, axis=1) == seg_rows[c]
        gm[c] = jnp.where(jnp.logical_and(ri >= ci, same), scores, 0.0)
    d_own = e_rows[0] * e_rows[1]
    dec[0:1, :] = e_rows[0]
    dec[1:2, :] = e_rows[1]
    dpair[core] = jnp.broadcast_to(d_own, (8, LANES))

    pair_send = pltpu.make_async_remote_copy(
        src_ref=dpair.at[core], dst_ref=dpair.at[core], send_sem=dps_sem, recv_sem=dp_sem,
        device_id=dev(partner), device_id_type=MESH)
    pair_send.start()

    def send_decays():
        pair_send.wait()
        dchip[...] = dpair[0] * dpair[1]
        dg[chip] = dpair[0] * dpair[1]
        dec[2:3, :] = dpair[0][0:1]
        dec[3:4, :] = dpair[1][0:1]

        @pl.loop(1, n_chip)
        def _(r):
            q = lax.rem(chip + r, n_chip)
            pltpu.make_async_remote_copy(
                src_ref=dchip, dst_ref=dg.at[chip], send_sem=dgs_sem, recv_sem=dg_sem,
                device_id=dev(2 * q + core), device_id_type=MESH).start()

    def expand(v, b):
        n = v.shape[0]
        r = pltpu.roll(v, lax.rem(2 * LANES - hb * b, LANES), 1)
        low = lax.broadcasted_iota(jnp.int32, (n, LANES), 1) < head_dim
        out = []
        for p in range(n_lt):
            out.append(jnp.where(low, jnp.broadcast_to(r[:, 2 * p:2 * p + 1], (n, LANES)),
                                 jnp.broadcast_to(r[:, 2 * p + 1:2 * p + 2], (n, LANES))))
        return jnp.concatenate(out, axis=1)

    def roll_to(dst, src, b):
        sh = lax.rem(2 * LANES - hb * b, LANES)
        for q in range(n_tok // LANES):
            dst[q * LANES:(q + 1) * LANES, :] = pltpu.roll(src[q * LANES:(q + 1) * LANES, :], sh, 1)

    low_r = lax.broadcasted_iota(jnp.int32, (ROWS, LANES), 1) < head_dim

    def head_cols(r0, lt):
        wv = arl[pl.ds(r0, ROWS), :]
        return jnp.where(low_r, jnp.broadcast_to(wv[:, 2 * lt:2 * lt + 1], (ROWS, LANES)),
                         jnp.broadcast_to(wv[:, 2 * lt + 1:2 * lt + 2], (ROWS, LANES)))

    def ublock(t_next, u_next, u_ref, b, t_ref):
        wnext(t_next)
        slot = lax.rem(t_next, 3)
        roll_to(arl, we, b)
        udot(slot, u_next)
        for r0 in range(0, n_tok, ROWS):
            for lt in range(n_lt):
                cols = slice(lt * LANES, (lt + 1) * LANES)
                xs = conv(u_ref, r0, lt, b * LB + lt * LANES).astype(BF16)
                xb[b, r0:r0 + ROWS, cols] = xs
                sc[r0:r0 + ROWS, cols] = (xs.astype(F32) * head_cols(r0, lt)).astype(BF16)

        ex = expand(dec[...], b)
        st0 = dot(bt[0], sc[0:CHUNK])
        cs0[b] = st0
        t_ref[...] = ex[1:2] * st0 + dot(bt[1], sc[CHUNK:2 * CHUNK])

    def part_copy(i):
        return pltpu.make_async_remote_copy(
            src_ref=tsend.at[i], dst_ref=two.at[i, core], send_sem=ps_sem.at[i], recv_sem=pr_sem.at[i],
            device_id=dev(partner), device_id_type=MESH)

    def home_copy(i, q):
        return pltpu.make_async_remote_copy(
            src_ref=tc.at[i, q], dst_ref=hrecv.at[i, chip], send_sem=s1_sem.at[i], recv_sem=r1_sem.at[i],
            device_id=dev(2 * q + core), device_id_type=MESH)

    def back_copy(i, q):
        return pltpu.make_async_remote_copy(
            src_ref=hout.at[i, q], dst_ref=s0r.at[i, chip], send_sem=s2_sem.at[i], recv_sem=r2_sem.at[i],
            device_id=dev(2 * q + core), device_id_type=MESH)

    def all_copies(src, dst, send_sem, recv_sem):
        return pltpu.make_async_remote_copy(
            src_ref=src.at[pl.ds(0, n_chip - 1)], dst_ref=dst.at[pl.ds(0, n_chip - 1)], send_sem=send_sem, recv_sem=recv_sem,
            device_id=dev(partner), device_id_type=MESH)

    def fin_copy(i):
        return pltpu.make_async_remote_copy(
            src_ref=fbuf.at[i, 1 - core], dst_ref=soth.at[i], send_sem=fs_sem.at[i], recv_sem=fr_sem.at[i],
            device_id=dev(partner), device_id_type=MESH)

    def send_home(i, b):
        part_copy(i).wait_recv()
        ex = expand(dec[...], b)
        for q in range(n_chip):
            rows = slice(q * hrows, (q + 1) * hrows)
            tc[i, q] = ex[3:4] * two[i, 0, rows] + two[i, 1, rows]
        hrecv[i, chip] = tc[i, chip]

        @pl.loop(1, n_chip, unroll=True)
        def _(r):
            home_copy(i, lax.rem(chip + r, n_chip)).start()

    def home(i):
        b = 2 * i + core
        all_copies(tc.at[i], hrecv.at[i], s1_sem.at[i], r1_sem.at[i]).wait_recv()
        run = jnp.zeros((hrows, LB), F32)
        for q in range(n_chip):
            hout[i, q] = run
            run = expand(dg[q], b)[0:1] * run + hrecv[i, q]
        s0r[i, chip] = hout[i, chip]

        @pl.loop(1, n_chip, unroll=True)
        def _(r):
            back_copy(i, lax.rem(chip + r, n_chip)).start()

    def finish(i):
        b = 2 * i + core
        all_copies(hout.at[i], s0r.at[i], s2_sem.at[i], r2_sem.at[i]).wait_recv()
        ex = expand(dec[...], b)
        for q in range(n_chip):
            rows = slice(q * hrows, (q + 1) * hrows)
            fbuf[i, 0, rows] = s0r[i, q]
            fbuf[i, 1, rows] = ex[2:3] * s0r[i, q] + two[i, 0, rows]
        fin_copy(i).start()

    @pl.loop(0, npair)
    def _(i):
        t = n_zfirst + 2 * i
        ublock(t + 1, us2, us, 2 * i + 1 - core, tsend.at[i])
        part_copy(i).start()

        @pl.when(i == 0)
        def _():
            send_decays()

        ublock(t + 2, us, us2, 2 * i + core, two.at[i, core])
        send_home(i, 2 * i + core)

        @pl.when(i == 0)
        def _():
            all_copies(dg, dg, dgs_sem, dg_sem).wait_recv()

        @pl.when(i >= 1)
        def _():
            home(i - 1)

        @pl.when(i >= 3)
        def _():
            finish(i - 3)

    for lt in range(n_lt):
        zb[n_zfirst, :, lt * LANES:(lt + 1) * LANES] = us[lt, HALO:HALO + n_tok, :].astype(BF16)

    low_b = (lax.broadcasted_iota(jnp.int32, (CHUNK, LANES), 1) < head_dim).astype(F32).astype(BF16)
    high_b = (lax.broadcasted_iota(jnp.int32, (CHUNK, LANES), 1) >= head_dim).astype(F32).astype(BF16)

    sub = 32

    def intra(b):
        heads = pl.ds(pl.multiple_of(b * hb, hb), hb)
        dsk = expand(prm[...], b)[2:3]
        for c in range(n_chunks):
            r0 = c * CHUNK
            ap8 = apt[heads, r0:r0 + CHUNK]
            ld8 = ldt[heads, r0:r0 + CHUNK]
            for p in range(n_lt):
                cols = slice(p * LANES, (p + 1) * LANES)
                k = p % 4
                for hh in range(2):
                    h = 2 * p + hh
                    aj0, aj1 = ap8[h:h + 1, :HALF], ap8[h:h + 1, HALF:]
                    ld0, ld1 = ld8[h:h + 1, :HALF], ld8[h:h + 1, HALF:]
                    base = CHUNK + hh * CHUNK
                    for q in range(HALF // sub):
                        rr = slice(q * sub, (q + 1) * sub)
                        g0 = slice(q * sub, (q + 1) * sub)
                        g1 = slice(HALF + q * sub, HALF + (q + 1) * sub)
                        ai0 = jnp.broadcast_to(arl[r0 + q * sub:r0 + (q + 1) * sub, h:h + 1], (sub, HALF))
                        ai1 = jnp.broadcast_to(arl[r0 + HALF + q * sub:r0 + HALF + (q + 1) * sub, h:h + 1], (sub, HALF))
                        mix[k, rr, hh * HALF:(hh + 1) * HALF] = (jnp.exp2(jnp.minimum(ai0 - aj0, ld0)) * gm[c, g0, 0:HALF]).astype(BF16)
                        mix[k, rr, base:base + HALF] = (jnp.exp2(ai1 - aj0) * gm[c, g1, 0:HALF]).astype(BF16)
                        mix[k, rr, base + HALF:base + CHUNK] = (jnp.exp2(jnp.minimum(ai1 - aj1, ld1)) * gm[c, g1, HALF:CHUNK]).astype(BF16)
                xp = xb[b, r0:r0 + CHUNK, cols]
                xa, xh = xp * low_b, xp * high_b
                y0 = dot(mix[k, :, 0:CHUNK], jnp.concatenate([xa[:HALF], xh[:HALF]], axis=0))
                y1 = dot(mix[k, :, CHUNK:3 * CHUNK], jnp.concatenate([xa, xh], axis=0))
                yb[b, r0:r0 + HALF, cols] = y0 + dsk[:, cols] * xp[:HALF].astype(F32)
                yb[b, r0 + HALF:r0 + CHUNK, cols] = y1 + dsk[:, cols] * xp[HALF:].astype(F32)

    def zdot(t, zi):
        slot = lax.rem(t, 3)
        zb[zi] = dot_nt(xe[HALO:HALO + n_tok], wbuf[slot]).astype(BF16)

    @pl.loop(0, n_zmid)
    def _(m):
        t = t_z + 1 + m
        wnext(t)
        roll_to(arl, a2, m)
        zdot(t, n_zfirst + 2 * (m + 1))
        intra(m)

        @pl.when(m == 0)
        def _():
            finish(npair - 3)

        @pl.when(m == n_zmid - 1)
        def _():
            home(npair - 1)

    @pl.loop(n_zmid, nb)
    def _(m):
        roll_to(arl, a2, m)
        intra(m)

        @pl.when(m == nb - 4)
        def _():
            finish(npair - 2)

    ssq[...] = jnp.zeros((n_tok, LANES), F32)

    def close(b, s_ref):
        ex = expand(dec[...], b)
        roll_to(arl, ws, b)
        s_in = s_ref[...]
        yst[0:CHUNK, :] = dot(bc[0:CHUNK, state_dim:2 * state_dim], s_in.astype(BF16))
        s_mid = ex[0:1] * s_in + cs0[b]
        yst[CHUNK:2 * CHUNK, :] = dot(bc[CHUNK:2 * CHUNK, state_dim:2 * state_dim], s_mid.astype(BF16))

        @pl.loop(0, n_tok // ROWS, unroll=True)
        def _(q):
            rows = pl.ds(pl.multiple_of(q * ROWS, ROWS), ROWS)
            acc = ssq[rows, :]
            for lt in range(n_lt):
                cols = slice(lt * LANES, (lt + 1) * LANES)
                y = yb[b, rows, cols] + head_cols(q * ROWS, lt) * yst[rows, cols]
                gated = y * half_silu(zb[b, rows, cols].astype(F32) * 0.5)
                yb[b, rows, cols] = gated
                acc = acc + gated * gated
            ssq[rows, :] = acc

    @pl.loop(0, npair)
    def _(i):
        fin_copy(i).wait_recv()
        t = t_z + n_zmid + 1 + i

        @pl.when(i < n_zlast)
        def _():
            wnext(t)

        zdot(jnp.minimum(t, 2 * nb - 1), jnp.where(i < n_zlast, n_zfirst + 1 + 2 * i, nb))
        close(2 * i + core, fbuf.at[i, core])
        close(2 * i + 1 - core, soth.at[i])

        @pl.when(i == npair - 3)
        def _():
            finish(npair - 1)

    scale = lax.rsqrt(jnp.sum(ssq[...], axis=1, keepdims=True) * (1.0 / d_inner) + EPS)
    ssq[...] = jnp.broadcast_to(scale, (n_tok, LANES))

    n_out = d_model // LB

    def normalize(b):
        @pl.loop(0, n_tok // ROWS, unroll=True)
        def _(q):
            rows = pl.ds(pl.multiple_of(q * ROWS, ROWS), ROWS)
            sv = ssq[rows, :]
            for lt in range(n_lt):
                cols = slice(lt * LANES, (lt + 1) * LANES)
                nw = nw_ref[:, pl.ds(pl.multiple_of(b * LB + lt * LANES, LANES), LANES)]
                zb[b, rows, cols] = (yb[b, rows, cols] * sv * nw).astype(BF16)

    @pl.loop(0, n_out)
    def _(b):
        normalize(b)

    def project(b, first, last):
        wnext(b + 2 * nb)
        slot = lax.rem(b + 2 * nb, 3)
        for n in range(n_out):
            part = dot(zb[b], wbuf[slot, :, n * LB:(n + 1) * LB])
            if not first:
                part = yb[n] + part
            if last:
                xb[n] = part.astype(BF16)
            else:
                yb[n] = part

    def ocopy(n):
        return pltpu.make_async_copy(xb.at[n], o_hbm.at[:, n * LB:(n + 1) * LB], gsem.at[n])

    project(jnp.int32(0), True, False)

    @pl.loop(1, nb - 1)
    def _(b):
        @pl.when(b >= n_out - 1)
        def _():
            normalize(b + 1)
        project(b, False, False)

    project(jnp.int32(nb - 1), False, True)
    for n in range(n_out):
        ocopy(n).start()

    @pl.when(me < n_seq - 1)
    def _():
        halo_send.wait_send()

    all_copies(dg, dg, dgs_sem, dg_sem).wait_send()

    @pl.loop(0, npair)
    def _(i):
        part_copy(i).wait_send()
        all_copies(tc.at[i], hrecv.at[i], s1_sem.at[i], r1_sem.at[i]).wait_send()
        all_copies(hout.at[i], s0r.at[i], s2_sem.at[i], r2_sem.at[i]).wait_send()
        fin_copy(i).wait_send()

    for n in range(n_out):
        ocopy(n).wait()


def mixer(n_seq, x, doc_start, w_in, conv_w, conv_b, dt_bias, a_log, d_skip, norm_w, w_out):
    n_tok, d_model = x.shape
    d_inner = norm_w.shape[0] * norm_w.shape[1]
    n_heads = a_log.shape[0]
    state_dim = (conv_w.shape[1] - d_inner) // 2
    nb = d_inner // LB
    npair = nb // 2
    n_chip = n_seq // 2
    hrows = state_dim // n_chip
    dims = (n_seq, n_tok, d_model, d_inner, n_heads, state_dim)
    vmem = pl.BlockSpec(memory_space=pltpu.VMEM)
    anyspace = pl.BlockSpec(memory_space=pl.ANY)
    dma = pltpu.SemaphoreType.DMA
    scratch = [
        pltpu.VMEM((n_tok + HALO, d_model), BF16),
        pltpu.VMEM((3, LB, d_model), BF16),
        pltpu.VMEM((2 * state_dim + LANES, d_model), BF16),
        pltpu.VMEM((nb + 1, n_tok, LB), BF16),
        pltpu.VMEM((nb, n_tok, LB), BF16),
        pltpu.VMEM((nb, n_tok, LB), F32),
        pltpu.VMEM((LB // LANES, n_tok + HALO, LANES), F32),
        pltpu.VMEM((LB // LANES, n_tok + HALO, LANES), F32),
        pltpu.VMEM((n_tok, LB), F32),
        pltpu.VMEM((n_tok, LB), BF16),
        pltpu.VMEM((4, HALF, 3 * CHUNK), BF16),
        pltpu.VMEM((nb, state_dim, LB), F32),
        pltpu.VMEM((npair, state_dim, LB), F32),
        pltpu.VMEM((npair, 2, state_dim, LB), F32),
        pltpu.VMEM((npair, n_chip, hrows, LB), F32),
        pltpu.VMEM((npair, n_chip, hrows, LB), F32),
        pltpu.VMEM((npair, n_chip, hrows, LB), F32),
        pltpu.VMEM((npair, n_chip, hrows, LB), F32),
        pltpu.VMEM((npair, 2, state_dim, LB), F32),
        pltpu.VMEM((npair, state_dim, LB), F32),
        pltpu.VMEM((n_tok, 2 * state_dim), BF16),
        pltpu.VMEM((n_tok // CHUNK, state_dim, CHUNK), BF16),
        pltpu.VMEM((n_tok // CHUNK, CHUNK, CHUNK), F32),
        pltpu.VMEM((n_tok, LANES), F32),
        pltpu.VMEM((LANES, n_tok), F32),
        pltpu.VMEM((LANES, n_tok), F32),
        pltpu.VMEM((n_tok, LANES), F32),
        pltpu.VMEM((n_tok, LANES), F32),
        pltpu.VMEM((n_tok, LANES), F32),
        pltpu.VMEM((8, LANES), F32),
        pltpu.VMEM((8, LANES), F32),
        pltpu.VMEM((2, 8, LANES), F32),
        pltpu.VMEM((8, LANES), F32),
        pltpu.VMEM((n_chip, 8, LANES), F32),
        pltpu.VMEM((3, n_tok, LANES), F32),
        pltpu.VMEM((n_tok, LANES), F32),
        pltpu.VMEM((HALO, d_model), BF16),
        dma(()), dma((3,)), dma(()), dma(()), dma(()), dma(()), dma(()), dma(()), dma(()),
        dma((npair,)), dma((npair,)), dma((npair,)), dma((npair,)), dma((npair,)), dma((npair,)), dma((npair,)), dma((npair,)),
        dma((d_model // LB,)),
    ]
    return pl.pallas_call(
        functools.partial(mixer_kernel, dims),
        out_shape=jax.ShapeDtypeStruct((n_tok, d_model), BF16),
        in_specs=[anyspace, vmem, anyspace, anyspace, vmem, vmem, vmem, vmem, vmem, vmem],
        out_specs=anyspace,
        scratch_shapes=scratch,
        compiler_params=pltpu.CompilerParams(collective_id=0, has_side_effects=True, vmem_limit_bytes=66 * 1000 * 1000),
        name='mixer',
    )(x, doc_start.reshape(n_tok // LANES, LANES), w_in.T, w_out, conv_w, conv_b.reshape(-1, LANES), dt_bias.reshape(1, -1),
      a_log.reshape(1, -1), d_skip.reshape(1, -1), norm_w.reshape(1, -1))


def solution(mesh):
    n_seq = mesh.shape['sp']
    row_spec = P(('dp', 'sp'), None)
    tok_spec = P(('dp', 'sp'))

    def layer_shard(x, doc_start, w_in, conv_w, conv_b, dt_bias, a_log, d_skip, norm_w, w_out):
        return mixer(n_seq, x, doc_start, w_in, conv_w, conv_b, dt_bias, a_log, d_skip, norm_w, w_out)

    return jax.shard_map(layer_shard, mesh=mesh, in_specs=(row_spec, tok_spec, P(), P(), P(), P(), P(), P(), P(), P()), out_specs=row_spec, check_vma=False)
```

```python
import functools
import math

import jax
import jax.numpy as jnp
from jax import lax
from jax.experimental import pallas as pl
from jax.experimental.pallas import tpu as pltpu
from jax.sharding import PartitionSpec as P

CHUNK = 256
HALF = 128
EPS = 1e-5
LB = 512
LANES = 128
HALO = 16
ROWS = 64
LOG2E = math.log2(math.e)
MESH = pl.DeviceIdType.MESH
F32 = jnp.float32
BF16 = jnp.bfloat16


def dot(a, b):
    return jnp.dot(a, b, preferred_element_type=F32)


def dot_nt(a, b):
    return lax.dot_general(a, b, (((1,), (1,)), ((), ())), preferred_element_type=F32)


def split3(v):
    s1 = v.astype(BF16)
    r1 = v - s1.astype(F32)
    s2 = r1.astype(BF16)
    s3 = (r1 - s2.astype(F32)).astype(BF16)
    return s1, s2, s3


def half_silu(c):
    return c + c * jnp.tanh(c)


def mixer_kernel(dims, x_hbm, ds_ref, w_hbm, wo_hbm, cw_ref, cb_ref, dtb_ref, alog_ref, dsk_ref, nw_ref, o_hbm,
                 xe, wbuf, wbcd, zb, xb, yb, us, us2, yst, sc, mix, cs0, tsend, two, tc, hrecv, hout, s0r, fbuf, soth,
                 bc, bt, gm, a2, apt, ldt, we, ws, arl, arm, prm, dec, dpair, dchip, dg, dga, mk, ssq, hal,
                 xsem, wsem, bsem, hs_sem, hr_sem, dp_sem, dps_sem, dg_sem, dgs_sem,
                 ps_sem, pr_sem, s1_sem, r1_sem, s2_sem, r2_sem, fs_sem, fr_sem, gsem):
    n_seq, n_tok, d_model, d_inner, n_heads, state_dim = dims
    head_dim = d_inner // n_heads
    nb = d_inner // LB
    hb = LB // head_dim
    npair = nb // 2
    n_chip = n_seq // 2
    hrows = state_dim // n_chip
    n_bcd = 2 * state_dim + n_heads
    n_lt = LB // LANES
    n_zfirst = 2
    t_z = n_zfirst + nb
    n_zmid = npair - 2
    n_zlast = npair - 1

    me = lax.axis_index('sp')
    chip = me // 2
    core = lax.rem(me, 2)
    partner = chip * 2 + (1 - core)

    def dev(i):
        return {'sp': i}

    def wcol(t):
        i2 = t - n_zfirst
        pair = i2 // 2
        own = lax.rem(i2, 2)
        ub = 2 * pair + jnp.where(own == 0, 1 - core, core)
        zi = jnp.where(t <= t_z, n_zfirst, jnp.where(t <= t_z + n_zmid, n_zfirst + 2 * (t - t_z), n_zfirst + 1 + 2 * (t - t_z - n_zmid - 1)))
        col = jnp.where(t < n_zfirst, t * LB,
                        jnp.where(t < n_zfirst + nb, d_inner + ub * LB, zi * LB))
        return pl.multiple_of(col, LB)

    def wcopy(t):
        slot = lax.rem(t, 3)
        return pltpu.make_async_copy(w_hbm.at[pl.ds(wcol(t), LB)], wbuf.at[slot], wsem.at[slot])

    n_steps = 3 * nb

    def wnext(t):
        slot = lax.rem(t, 3)
        pltpu.make_async_copy(w_hbm.at[pl.ds(0, LB)], wbuf.at[slot], wsem.at[slot]).wait()

        @pl.when(t + 2 < 2 * nb)
        def _():
            wcopy(t + 2).start()

        @pl.when(jnp.logical_and(t + 2 >= 2 * nb, t + 2 < n_steps))
        def _():
            slot = lax.rem(t + 2, 3)
            pltpu.make_async_copy(wo_hbm.at[pl.ds(pl.multiple_of((t + 2 - 2 * nb) * LB, LB), LB)], wbuf.at[slot], wsem.at[slot]).start()

    xcopy = pltpu.make_async_copy(x_hbm, xe.at[pl.ds(HALO, n_tok)], xsem)
    xcopy.start()
    wcopy(jnp.int32(0)).start()
    bcopy = pltpu.make_async_copy(w_hbm.at[pl.ds(2 * d_inner, n_bcd)], wbcd.at[pl.ds(0, n_bcd)], bsem)
    bcopy.start()
    wbcd[n_bcd:, :] = jnp.zeros((LANES - n_heads, d_model), BF16)
    wcopy(jnp.int32(1)).start()

    barrier = pltpu.get_barrier_semaphore()
    pl.semaphore_signal(barrier, inc=1, device_id=dev(lax.rem(me + 1, n_seq)), device_id_type=MESH)
    pl.semaphore_signal(barrier, inc=1, device_id=dev(lax.rem(me + n_seq - 1, n_seq)), device_id_type=MESH)

    @pl.loop(1, n_chip)
    def _(r):
        pl.semaphore_signal(barrier, inc=1, device_id=dev(lax.rem(me + 2 * r, n_seq)), device_id_type=MESH)

    ri = lax.broadcasted_iota(jnp.int32, (CHUNK, CHUNK), 0)
    ci = lax.broadcasted_iota(jnp.int32, (CHUNK, CHUNK), 1)
    tri = (ri >= ci).astype(F32).astype(BF16)
    eye = (ri == ci).astype(F32).astype(BF16)
    n_chunks = n_tok // CHUNK
    per = CHUNK // LANES
    seg_cols, seg_rows, ds_cols = [], [], []
    for c in range(n_chunks):
        row = jnp.concatenate([ds_ref[per * c + q:per * c + q + 1, :] for q in range(per)], axis=1).astype(F32)
        row = jnp.broadcast_to(row, (8, CHUNK)).astype(BF16)
        ds_cols.append(jnp.broadcast_to(dot_nt(eye, row)[:, 0:1], (CHUNK, LANES)))
        seg_cols.append(jnp.broadcast_to(dot_nt(tri, row)[:, 0:1], (CHUNK, LANES)))
        seg_rows.append(dot_nt(row, tri)[0:1, :])
    keep = 1.0 - jnp.concatenate(ds_cols, axis=0)
    tok = lax.broadcasted_iota(jnp.int32, (n_tok, LANES), 0)
    m1 = keep
    k1 = jnp.where(tok >= 1, pltpu.roll(keep, 1, 0), 1.0)
    k2 = jnp.where(tok >= 2, pltpu.roll(keep, 2, 0), 1.0)
    mk[0] = m1
    mk[1] = m1 * k1
    mk[2] = m1 * k1 * k2

    xcopy.wait()
    hrow = lax.broadcasted_iota(jnp.int32, (HALO, LANES), 0)
    k_last = jnp.broadcast_to(mk[0, n_tok - 8:n_tok, :][7:8, :], (HALO, LANES))
    k_last2 = jnp.broadcast_to(mk[1, n_tok - 8:n_tok, :][7:8, :], (HALO, LANES))
    hmask = jnp.where(hrow == HALO - 1, 1.0, jnp.where(hrow == HALO - 2, k_last, jnp.where(hrow == HALO - 3, k_last2, 0.0)))
    for q in range(d_model // LANES):
        hal[:, q * LANES:(q + 1) * LANES] = (xe[n_tok:n_tok + HALO, q * LANES:(q + 1) * LANES].astype(F32) * hmask).astype(BF16)

    def zblock(t, zi):
        wnext(t)
        slot = lax.rem(t, 3)
        zb[zi] = dot_nt(xe[HALO:HALO + n_tok], wbuf[slot]).astype(BF16)

    pl.semaphore_wait(barrier, n_chip + 1)
    halo_send = pltpu.make_async_remote_copy(
        src_ref=hal, dst_ref=xe.at[pl.ds(0, HALO)], send_sem=hs_sem, recv_sem=hr_sem,
        device_id=dev(lax.rem(me + 1, n_seq)), device_id_type=MESH)

    @pl.when(me < n_seq - 1)
    def _():
        halo_send.start()

    @pl.when(me == 0)
    def _():
        xe[0:HALO, :] = jnp.zeros((HALO, d_model), BF16)

    @pl.loop(0, n_zfirst)
    def _(t):
        zblock(t, t)

    @pl.when(me > 0)
    def _():
        halo_send.wait_recv()

    bcopy.wait()
    lane = lax.broadcasted_iota(jnp.int32, (1, LANES), 1)
    p_bcd = dot_nt(xe[...], wbcd[...]).astype(BF16).astype(F32)
    for lt in range(2 * state_dim // LANES + 1):
        us2[lt] = p_bcd[:, lt * LANES:(lt + 1) * LANES]

    def udot(slot, u_ref):
        p_u = dot_nt(xe[...], wbuf[slot]).astype(BF16).astype(F32)
        for lt in range(n_lt):
            u_ref[lt] = p_u[:, lt * LANES:(lt + 1) * LANES]

    t_u = n_zfirst
    wnext(jnp.int32(t_u))
    udot(t_u % 3, us)

    def conv(u_ref, r0, lt, wl):
        wl = pl.multiple_of(wl, LANES)
        cw = cw_ref[:, pl.ds(wl, LANES)] * 0.5
        v = cb_ref[pl.ds(wl // LANES, 1), :] * 0.5 + cw[0:1] * u_ref[lt, pl.ds(r0 + HALO, ROWS), :]
        for k in range(1, 4):
            v = v + cw[k:k + 1] * (mk[k - 1, pl.ds(r0, ROWS), :] * u_ref[lt, pl.ds(r0 + HALO - k, ROWS), :])
        return half_silu(v)

    for r0 in range(0, n_tok, ROWS):
        for lt in range(2 * state_dim // LANES):
            bc[r0:r0 + ROWS, lt * LANES:(lt + 1) * LANES] = conv(us2, r0, lt, d_inner + lt * LANES).astype(BF16)

    prm[...] = jnp.zeros((8, LANES), F32)
    prm[0:1, 0:n_heads] = dtb_ref[...]
    prm[1:2, 0:n_heads] = alog_ref[...]
    prm[2:3, 0:n_heads] = dsk_ref[...]
    pv = prm[...]
    head_ok = lane < n_heads
    neg_a = jnp.where(head_ok, -jnp.exp(pv[1:2]) , 0.0)
    e_rows = []
    for c in range(n_chunks):
        rows = slice(c * CHUNK, (c + 1) * CHUNK)
        raw = jnp.where(head_ok, us2[2 * state_dim // LANES, HALO + c * CHUNK:HALO + (c + 1) * CHUNK, :], 0.0) + pv[0:1]
        dt = jnp.maximum(raw, 0.0) + jnp.log1p(jnp.exp(-jnp.abs(raw)))
        s1, s2, s3 = split3(neg_a * dt * LOG2E)
        acum = dot(tri, s3) + dot(tri, s2) + dot(tri, s1)
        a2[rows, :] = acum
        a_t = jnp.transpose(acum)
        ld_t = jnp.transpose(jnp.log2(dt))
        ldt[:, rows] = ld_t
        apt[:, rows] = a_t - ld_t
        seg = seg_cols[c]
        last = acum[CHUNK - 1:CHUNK, :]
        seg_last = seg[CHUNK - 1:CHUNK, :]
        ws[rows, :] = jnp.where(seg == 0.0, jnp.exp2(acum), 0.0)
        we[rows, :] = jnp.where(seg == seg_last, jnp.exp2(last - acum) * dt, 0.0)
        e_rows.append(jnp.where(seg_last == 0.0, jnp.exp2(last), 0.0))
        b_c = bc[rows, 0:state_dim]
        c_c = bc[rows, state_dim:2 * state_dim]
        b_t = jnp.transpose(b_c.astype(F32)).astype(BF16)
        bt[c] = b_t
        scores = dot(c_c, b_t)
        same = jnp.concatenate([seg] * per, axis=1) == seg_rows[c]
        gm[c] = jnp.where(jnp.logical_and(ri >= ci, same), scores, 0.0)
    d_own = e_rows[0] * e_rows[1]
    dec[0:1, :] = e_rows[0]
    dec[1:2, :] = e_rows[1]
    dpair[core] = jnp.broadcast_to(d_own, (8, LANES))

    pair_send = pltpu.make_async_remote_copy(
        src_ref=dpair.at[core], dst_ref=dpair.at[core], send_sem=dps_sem, recv_sem=dp_sem,
        device_id=dev(partner), device_id_type=MESH)
    pair_send.start()

    def send_decays():
        pair_send.wait()
        dchip[...] = dpair[0] * dpair[1]
        dg[chip] = dpair[0] * dpair[1]
        dec[2:3, :] = dpair[0][0:1]
        dec[3:4, :] = dpair[1][0:1]

        @pl.loop(1, n_chip)
        def _(r):
            q = lax.rem(chip + r, n_chip)
            pltpu.make_async_remote_copy(
                src_ref=dchip, dst_ref=dg.at[chip], send_sem=dgs_sem, recv_sem=dg_sem,
                device_id=dev(2 * q + core), device_id_type=MESH).start()

    def expand(v, b):
        n = v.shape[0]
        r = pltpu.roll(v, lax.rem(2 * LANES - hb * b, LANES), 1)
        low = lax.broadcasted_iota(jnp.int32, (n, LANES), 1) < head_dim
        out = []
        for p in range(n_lt):
            out.append(jnp.where(low, jnp.broadcast_to(r[:, 2 * p:2 * p + 1], (n, LANES)),
                                 jnp.broadcast_to(r[:, 2 * p + 1:2 * p + 2], (n, LANES))))
        return jnp.concatenate(out, axis=1)

    def roll_to(dst, src, b):
        sh = lax.rem(2 * LANES - hb * b, LANES)
        for q in range(n_tok // LANES):
            dst[q * LANES:(q + 1) * LANES, :] = pltpu.roll(src[q * LANES:(q + 1) * LANES, :], sh, 1)

    low_r = lax.broadcasted_iota(jnp.int32, (ROWS, LANES), 1) < head_dim

    def head_cols(r0, lt):
        wv = arl[pl.ds(r0, ROWS), :]
        return jnp.where(low_r, jnp.broadcast_to(wv[:, 2 * lt:2 * lt + 1], (ROWS, LANES)),
                         jnp.broadcast_to(wv[:, 2 * lt + 1:2 * lt + 2], (ROWS, LANES)))

    low_b = (lax.broadcasted_iota(jnp.int32, (CHUNK, LANES), 1) < head_dim).astype(F32).astype(BF16)
    high_b = (lax.broadcasted_iota(jnp.int32, (CHUNK, LANES), 1) >= head_dim).astype(F32).astype(BF16)

    sub = 32

    def intra(b):
        roll_to(arm, a2, b)
        heads = pl.ds(pl.multiple_of(b * hb, hb), hb)
        dsk = expand(prm[...], b)[2:3]
        for c in range(n_chunks):
            r0 = c * CHUNK
            ap8 = apt[heads, r0:r0 + CHUNK]
            ld8 = ldt[heads, r0:r0 + CHUNK]
            for p in range(n_lt):
                cols = slice(p * LANES, (p + 1) * LANES)
                k = p % 4
                for hh in range(2):
                    h = 2 * p + hh
                    aj0, aj1 = ap8[h:h + 1, :HALF], ap8[h:h + 1, HALF:]
                    ld0, ld1 = ld8[h:h + 1, :HALF], ld8[h:h + 1, HALF:]
                    base = CHUNK + hh * CHUNK
                    for q in range(HALF // sub):
                        rr = slice(q * sub, (q + 1) * sub)
                        g0 = slice(q * sub, (q + 1) * sub)
                        g1 = slice(HALF + q * sub, HALF + (q + 1) * sub)
                        ai0 = jnp.broadcast_to(arm[r0 + q * sub:r0 + (q + 1) * sub, h:h + 1], (sub, HALF))
                        ai1 = jnp.broadcast_to(arm[r0 + HALF + q * sub:r0 + HALF + (q + 1) * sub, h:h + 1], (sub, HALF))
                        mix[k, rr, hh * HALF:(hh + 1) * HALF] = (jnp.exp2(jnp.minimum(ai0 - aj0, ld0)) * gm[c, g0, 0:HALF]).astype(BF16)
                        mix[k, rr, base:base + HALF] = (jnp.exp2(ai1 - aj0) * gm[c, g1, 0:HALF]).astype(BF16)
                        mix[k, rr, base + HALF:base + CHUNK] = (jnp.exp2(jnp.minimum(ai1 - aj1, ld1)) * gm[c, g1, HALF:CHUNK]).astype(BF16)
                xp = xb[b, r0:r0 + CHUNK, cols]
                xa, xh = xp * low_b, xp * high_b
                y0 = dot(mix[k, :, 0:CHUNK], jnp.concatenate([xa[:HALF], xh[:HALF]], axis=0))
                y1 = dot(mix[k, :, CHUNK:3 * CHUNK], jnp.concatenate([xa, xh], axis=0))
                yb[b, r0:r0 + HALF, cols] = y0 + dsk[:, cols] * xp[:HALF].astype(F32)
                yb[b, r0 + HALF:r0 + CHUNK, cols] = y1 + dsk[:, cols] * xp[HALF:].astype(F32)

    def ublock(t_next, u_next, u_ref, b, t_ref, b_done):
        wnext(t_next)
        slot = lax.rem(t_next, 3)
        roll_to(arl, we, b)
        udot(slot, u_next)
        for r0 in range(0, n_tok, ROWS):
            for lt in range(n_lt):
                cols = slice(lt * LANES, (lt + 1) * LANES)
                xs = conv(u_ref, r0, lt, b * LB + lt * LANES).astype(BF16)
                xb[b, r0:r0 + ROWS, cols] = xs
                sc[r0:r0 + ROWS, cols] = (xs.astype(F32) * head_cols(r0, lt)).astype(BF16)

        intra(b_done)
        ex = expand(dec[...], b)
        st0 = dot(bt[0], sc[0:CHUNK])
        cs0[b] = st0
        t_ref[...] = ex[1:2] * st0 + dot(bt[1], sc[CHUNK:2 * CHUNK])

    def part_copy(i):
        return pltpu.make_async_remote_copy(
            src_ref=tsend.at[i], dst_ref=two.at[i, core], send_sem=ps_sem.at[i], recv_sem=pr_sem.at[i],
            device_id=dev(partner), device_id_type=MESH)

    def home_copy(i, q):
        return pltpu.make_async_remote_copy(
            src_ref=tc.at[i, q], dst_ref=hrecv.at[i, chip], send_sem=s1_sem.at[i], recv_sem=r1_sem.at[i],
            device_id=dev(2 * q + core), device_id_type=MESH)

    def back_copy(i, q):
        return pltpu.make_async_remote_copy(
            src_ref=hout.at[i, q], dst_ref=s0r.at[i, chip], send_sem=s2_sem.at[i], recv_sem=r2_sem.at[i],
            device_id=dev(2 * q + core), device_id_type=MESH)

    def all_copies(src, dst, send_sem, recv_sem):
        return pltpu.make_async_remote_copy(
            src_ref=src.at[pl.ds(0, n_chip - 1)], dst_ref=dst.at[pl.ds(0, n_chip - 1)], send_sem=send_sem, recv_sem=recv_sem,
            device_id=dev(partner), device_id_type=MESH)

    def fin_copy(i):
        return pltpu.make_async_remote_copy(
            src_ref=fbuf.at[i, 1 - core], dst_ref=soth.at[i], send_sem=fs_sem.at[i], recv_sem=fr_sem.at[i],
            device_id=dev(partner), device_id_type=MESH)

    def send_home(i, b):
        part_copy(i).wait_recv()
        ex = expand(dec[...], b)
        for q in range(n_chip):
            rows = slice(q * hrows, (q + 1) * hrows)
            tc[i, q] = ex[3:4] * two[i, 0, rows] + two[i, 1, rows]
        hrecv[i, chip] = tc[i, chip]

        @pl.loop(1, n_chip, unroll=True)
        def _(r):
            home_copy(i, lax.rem(chip + r, n_chip)).start()

    def home(i):
        b = 2 * i + core
        all_copies(tc.at[i], hrecv.at[i], s1_sem.at[i], r1_sem.at[i]).wait_recv()
        ex = expand(dga[...], b)
        run = jnp.zeros((hrows, LB), F32)
        for q in range(n_chip):
            hout[i, q] = run
            run = ex[q:q + 1] * run + hrecv[i, q]
        s0r[i, chip] = hout[i, chip]

        @pl.loop(1, n_chip, unroll=True)
        def _(r):
            back_copy(i, lax.rem(chip + r, n_chip)).start()

    def finish(i):
        b = 2 * i + core
        all_copies(hout.at[i], s0r.at[i], s2_sem.at[i], r2_sem.at[i]).wait_recv()
        ex = expand(dec[...], b)
        for q in range(n_chip):
            rows = slice(q * hrows, (q + 1) * hrows)
            fbuf[i, 0, rows] = s0r[i, q]
            fbuf[i, 1, rows] = ex[2:3] * s0r[i, q] + two[i, 0, rows]
        fin_copy(i).start()

    @pl.loop(0, npair)
    def _(i):
        t = n_zfirst + 2 * i
        ublock(t + 1, us2, us, 2 * i + 1 - core, tsend.at[i], 2 * jnp.maximum(i - 1, 0) + core)
        part_copy(i).start()

        @pl.when(i == 0)
        def _():
            send_decays()

        ublock(t + 2, us, us2, 2 * i + core, two.at[i, core], 2 * i + 1 - core)
        send_home(i, 2 * i + core)

        @pl.when(i == 0)
        def _():
            all_copies(dg, dg, dgs_sem, dg_sem).wait_recv()
            for q in range(n_chip):
                dga[q:q + 1, :] = dg[q, 0:1, :]

        @pl.when(i >= 1)
        def _():
            home(i - 1)

        @pl.when(i >= 3)
        def _():
            finish(i - 3)

    for lt in range(n_lt):
        zb[n_zfirst, :, lt * LANES:(lt + 1) * LANES] = us[lt, HALO:HALO + n_tok, :].astype(BF16)

    def zdot(t, zi):
        slot = lax.rem(t, 3)
        zb[zi] = dot_nt(xe[HALO:HALO + n_tok], wbuf[slot]).astype(BF16)

    @pl.loop(0, n_zmid)
    def _(m):
        t = t_z + 1 + m
        wnext(t)
        zdot(t, n_zfirst + 2 * (m + 1))

        @pl.when(m == 0)
        def _():
            finish(npair - 3)

        @pl.when(m == 1)
        def _():
            intra(2 * (npair - 1) + core)

        @pl.when(m == n_zmid - 1)
        def _():
            home(npair - 1)

    ssq[...] = jnp.zeros((n_tok, LANES), F32)

    def close(b, s_ref):
        ex = expand(dec[...], b)
        roll_to(arl, ws, b)
        s_in = s_ref[...]
        yst[0:CHUNK, :] = dot(bc[0:CHUNK, state_dim:2 * state_dim], s_in.astype(BF16))
        s_mid = ex[0:1] * s_in + cs0[b]
        yst[CHUNK:2 * CHUNK, :] = dot(bc[CHUNK:2 * CHUNK, state_dim:2 * state_dim], s_mid.astype(BF16))

        @pl.loop(0, n_tok // ROWS, unroll=True)
        def _(q):
            rows = pl.ds(pl.multiple_of(q * ROWS, ROWS), ROWS)
            acc = ssq[rows, :]
            for lt in range(n_lt):
                cols = slice(lt * LANES, (lt + 1) * LANES)
                y = yb[b, rows, cols] + head_cols(q * ROWS, lt) * yst[rows, cols]
                gated = y * half_silu(zb[b, rows, cols].astype(F32) * 0.5)
                yb[b, rows, cols] = gated
                acc = acc + gated * gated
            ssq[rows, :] = acc

    @pl.loop(0, npair)
    def _(i):
        fin_copy(i).wait_recv()
        t = t_z + n_zmid + 1 + i

        @pl.when(i < n_zlast)
        def _():
            wnext(t)

        zdot(jnp.minimum(t, 2 * nb - 1), jnp.where(i < n_zlast, n_zfirst + 1 + 2 * i, nb))
        close(2 * i + core, fbuf.at[i, core])
        close(2 * i + 1 - core, soth.at[i])

        @pl.when(i == 0)
        def _():
            finish(npair - 2)

        @pl.when(i == npair - 3)
        def _():
            finish(npair - 1)

    scale = lax.rsqrt(jnp.sum(ssq[...], axis=1, keepdims=True) * (1.0 / d_inner) + EPS)
    ssq[...] = jnp.broadcast_to(scale, (n_tok, LANES))

    n_out = d_model // LB

    def normalize(b):
        @pl.loop(0, n_tok // ROWS, unroll=True)
        def _(q):
            rows = pl.ds(pl.multiple_of(q * ROWS, ROWS), ROWS)
            sv = ssq[rows, :]
            for lt in range(n_lt):
                cols = slice(lt * LANES, (lt + 1) * LANES)
                nw = nw_ref[:, pl.ds(pl.multiple_of(b * LB + lt * LANES, LANES), LANES)]
                zb[b, rows, cols] = (yb[b, rows, cols] * sv * nw).astype(BF16)

    @pl.loop(0, n_out)
    def _(b):
        normalize(b)

    def ocopy(n):
        return pltpu.make_async_copy(xb.at[n], o_hbm.at[:, n * LB:(n + 1) * LB], gsem.at[n])

    def project(b, first, last):
        wnext(b + 2 * nb)
        slot = lax.rem(b + 2 * nb, 3)
        for n in range(n_out):
            part = dot(zb[b], wbuf[slot, :, n * LB:(n + 1) * LB])
            if not first:
                part = yb[n] + part
            if last:
                xb[n] = part.astype(BF16)
                ocopy(n).start()
            else:
                yb[n] = part

    project(jnp.int32(0), True, False)

    @pl.loop(1, nb - 1)
    def _(b):
        @pl.when(b >= n_out - 1)
        def _():
            normalize(b + 1)
        project(b, False, False)

    project(jnp.int32(nb - 1), False, True)

    @pl.when(me < n_seq - 1)
    def _():
        halo_send.wait_send()

    all_copies(dg, dg, dgs_sem, dg_sem).wait_send()

    @pl.loop(0, npair)
    def _(i):
        part_copy(i).wait_send()
        all_copies(tc.at[i], hrecv.at[i], s1_sem.at[i], r1_sem.at[i]).wait_send()
        all_copies(hout.at[i], s0r.at[i], s2_sem.at[i], r2_sem.at[i]).wait_send()
        fin_copy(i).wait_send()

    for n in range(n_out):
        ocopy(n).wait()


def mixer(n_seq, x, doc_start, w_in, conv_w, conv_b, dt_bias, a_log, d_skip, norm_w, w_out):
    n_tok, d_model = x.shape
    d_inner = norm_w.shape[0] * norm_w.shape[1]
    n_heads = a_log.shape[0]
    state_dim = (conv_w.shape[1] - d_inner) // 2
    nb = d_inner // LB
    npair = nb // 2
    n_chip = n_seq // 2
    hrows = state_dim // n_chip
    dims = (n_seq, n_tok, d_model, d_inner, n_heads, state_dim)
    vmem = pl.BlockSpec(memory_space=pltpu.VMEM)
    anyspace = pl.BlockSpec(memory_space=pl.ANY)
    dma = pltpu.SemaphoreType.DMA
    scratch = [
        pltpu.VMEM((n_tok + HALO, d_model), BF16),
        pltpu.VMEM((3, LB, d_model), BF16),
        pltpu.VMEM((2 * state_dim + LANES, d_model), BF16),
        pltpu.VMEM((nb + 1, n_tok, LB), BF16),
        pltpu.VMEM((nb, n_tok, LB), BF16),
        pltpu.VMEM((nb, n_tok, LB), F32),
        pltpu.VMEM((LB // LANES, n_tok + HALO, LANES), F32),
        pltpu.VMEM((LB // LANES, n_tok + HALO, LANES), F32),
        pltpu.VMEM((n_tok, LB), F32),
        pltpu.VMEM((n_tok, LB), BF16),
        pltpu.VMEM((4, HALF, 3 * CHUNK), BF16),
        pltpu.VMEM((nb, state_dim, LB), F32),
        pltpu.VMEM((npair, state_dim, LB), F32),
        pltpu.VMEM((npair, 2, state_dim, LB), F32),
        pltpu.VMEM((npair, n_chip, hrows, LB), F32),
        pltpu.VMEM((npair, n_chip, hrows, LB), F32),
        pltpu.VMEM((npair, n_chip, hrows, LB), F32),
        pltpu.VMEM((npair, n_chip, hrows, LB), F32),
        pltpu.VMEM((npair, 2, state_dim, LB), F32),
        pltpu.VMEM((npair, state_dim, LB), F32),
        pltpu.VMEM((n_tok, 2 * state_dim), BF16),
        pltpu.VMEM((n_tok // CHUNK, state_dim, CHUNK), BF16),
        pltpu.VMEM((n_tok // CHUNK, CHUNK, CHUNK), F32),
        pltpu.VMEM((n_tok, LANES), F32),
        pltpu.VMEM((LANES, n_tok), F32),
        pltpu.VMEM((LANES, n_tok), F32),
        pltpu.VMEM((n_tok, LANES), F32),
        pltpu.VMEM((n_tok, LANES), F32),
        pltpu.VMEM((n_tok, LANES), F32),
        pltpu.VMEM((n_tok, LANES), F32),
        pltpu.VMEM((8, LANES), F32),
        pltpu.VMEM((8, LANES), F32),
        pltpu.VMEM((2, 8, LANES), F32),
        pltpu.VMEM((8, LANES), F32),
        pltpu.VMEM((n_chip, 8, LANES), F32),
        pltpu.VMEM((n_chip, LANES), F32),
        pltpu.VMEM((3, n_tok, LANES), F32),
        pltpu.VMEM((n_tok, LANES), F32),
        pltpu.VMEM((HALO, d_model), BF16),
        dma(()), dma((3,)), dma(()), dma(()), dma(()), dma(()), dma(()), dma(()), dma(()),
        dma((npair,)), dma((npair,)), dma((npair,)), dma((npair,)), dma((npair,)), dma((npair,)), dma((npair,)), dma((npair,)),
        dma((d_model // LB,)),
    ]
    return pl.pallas_call(
        functools.partial(mixer_kernel, dims),
        out_shape=jax.ShapeDtypeStruct((n_tok, d_model), BF16),
        in_specs=[anyspace, vmem, anyspace, anyspace, vmem, vmem, vmem, vmem, vmem, vmem],
        out_specs=anyspace,
        scratch_shapes=scratch,
        compiler_params=pltpu.CompilerParams(collective_id=0, has_side_effects=True, vmem_limit_bytes=66 * 1000 * 1000),
        name='mixer',
    )(x, doc_start.reshape(n_tok // LANES, LANES), w_in.T, w_out, conv_w, conv_b.reshape(-1, LANES), dt_bias.reshape(1, -1),
      a_log.reshape(1, -1), d_skip.reshape(1, -1), norm_w.reshape(1, -1))


def solution(mesh):
    n_seq = mesh.shape['sp']
    row_spec = P(('dp', 'sp'), None)
    tok_spec = P(('dp', 'sp'))

    def layer_shard(x, doc_start, w_in, conv_w, conv_b, dt_bias, a_log, d_skip, norm_w, w_out):
        return mixer(n_seq, x, doc_start, w_in, conv_w, conv_b, dt_bias, a_log, d_skip, norm_w, w_out)

    return jax.shard_map(layer_shard, mesh=mesh, in_specs=(row_spec, tok_spec, P(), P(), P(), P(), P(), P(), P(), P()), out_specs=row_spec, check_vma=False)
```

```python
import functools
import math

import jax
import jax.numpy as jnp
from jax import lax
from jax.experimental import pallas as pl
from jax.experimental.pallas import tpu as pltpu
from jax.sharding import PartitionSpec as P

CHUNK = 256
HALF = 128
EPS = 1e-5
LB = 512
LANES = 128
HALO = 16
ROWS = 64
LOG2E = math.log2(math.e)
MESH = pl.DeviceIdType.MESH
F32 = jnp.float32
BF16 = jnp.bfloat16


def dot(a, b):
    return jnp.dot(a, b, preferred_element_type=F32)


def dot_nt(a, b):
    return lax.dot_general(a, b, (((1,), (1,)), ((), ())), preferred_element_type=F32)


def split3(v):
    s1 = v.astype(BF16)
    r1 = v - s1.astype(F32)
    s2 = r1.astype(BF16)
    s3 = (r1 - s2.astype(F32)).astype(BF16)
    return s1, s2, s3


def half_silu(c):
    return c + c * jnp.tanh(c)


def mixer_kernel(dims, x_hbm, ds_ref, w_hbm, wo_hbm, cw_ref, cb_ref, dtb_ref, alog_ref, dsk_ref, nw_ref, o_hbm,
                 xe, wbuf, wbcd, zb, xb, yb, us, us2, yst, sc, mix, cs0, tsend, two, tc, hrecv, hout, s0r, fbuf, soth,
                 bc, bt, gm, a2, apt, ldt, we, ws, arl, arm, prm, dec, dpair, dchip, dg, dga, mk, ssq, hal,
                 xsem, wsem, bsem, hs_sem, hr_sem, dp_sem, dps_sem, dg_sem, dgs_sem,
                 ps_sem, pr_sem, s1_sem, r1_sem, s2_sem, r2_sem, fs_sem, fr_sem, gsem):
    n_seq, n_tok, d_model, d_inner, n_heads, state_dim = dims
    head_dim = d_inner // n_heads
    nb = d_inner // LB
    hb = LB // head_dim
    npair = nb // 2
    n_chip = n_seq // 2
    hrows = state_dim // n_chip
    n_bcd = 2 * state_dim + n_heads
    n_lt = LB // LANES
    n_zfirst = 2
    t_z = n_zfirst + nb
    n_zmid = npair - 2
    n_zlast = npair - 1

    me = lax.axis_index('sp')
    chip = me // 2
    core = lax.rem(me, 2)
    partner = chip * 2 + (1 - core)

    def dev(i):
        return {'sp': i}

    def wcol(t):
        i2 = t - n_zfirst
        pair = i2 // 2
        own = lax.rem(i2, 2)
        ub = 2 * pair + jnp.where(own == 0, 1 - core, core)
        zi = jnp.where(t <= t_z, n_zfirst, jnp.where(t <= t_z + n_zmid, n_zfirst + 2 * (t - t_z), n_zfirst + 1 + 2 * (t - t_z - n_zmid - 1)))
        col = jnp.where(t < n_zfirst, t * LB,
                        jnp.where(t < n_zfirst + nb, d_inner + ub * LB, zi * LB))
        return pl.multiple_of(col, LB)

    def wcopy(t):
        slot = lax.rem(t, 3)
        return pltpu.make_async_copy(w_hbm.at[pl.ds(wcol(t), LB)], wbuf.at[slot], wsem.at[slot])

    n_steps = 3 * nb

    def wnext(t):
        slot = lax.rem(t, 3)
        pltpu.make_async_copy(w_hbm.at[pl.ds(0, LB)], wbuf.at[slot], wsem.at[slot]).wait()

        @pl.when(t + 2 < 2 * nb)
        def _():
            wcopy(t + 2).start()

        @pl.when(jnp.logical_and(t + 2 >= 2 * nb, t + 2 < n_steps))
        def _():
            slot = lax.rem(t + 2, 3)
            pltpu.make_async_copy(wo_hbm.at[pl.ds(pl.multiple_of((t + 2 - 2 * nb) * LB, LB), LB)], wbuf.at[slot], wsem.at[slot]).start()

    xcopy = pltpu.make_async_copy(x_hbm, xe.at[pl.ds(HALO, n_tok)], xsem)
    xcopy.start()
    wcopy(jnp.int32(0)).start()
    bcopy = pltpu.make_async_copy(w_hbm.at[pl.ds(2 * d_inner, n_bcd)], wbcd.at[pl.ds(0, n_bcd)], bsem)
    wbcd[n_bcd:, :] = jnp.zeros((LANES - n_heads, d_model), BF16)

    barrier = pltpu.get_barrier_semaphore()
    pl.semaphore_signal(barrier, inc=1, device_id=dev(lax.rem(me + 1, n_seq)), device_id_type=MESH)
    pl.semaphore_signal(barrier, inc=1, device_id=dev(lax.rem(me + n_seq - 1, n_seq)), device_id_type=MESH)

    @pl.loop(1, n_chip)
    def _(r):
        pl.semaphore_signal(barrier, inc=1, device_id=dev(lax.rem(me + 2 * r, n_seq)), device_id_type=MESH)

    ri = lax.broadcasted_iota(jnp.int32, (CHUNK, CHUNK), 0)
    ci = lax.broadcasted_iota(jnp.int32, (CHUNK, CHUNK), 1)
    tri = (ri >= ci).astype(F32).astype(BF16)
    eye = (ri == ci).astype(F32).astype(BF16)
    n_chunks = n_tok // CHUNK
    per = CHUNK // LANES
    seg_cols, seg_rows, ds_cols = [], [], []
    for c in range(n_chunks):
        row = jnp.concatenate([ds_ref[per * c + q:per * c + q + 1, :] for q in range(per)], axis=1).astype(F32)
        row = jnp.broadcast_to(row, (8, CHUNK)).astype(BF16)
        ds_cols.append(jnp.broadcast_to(dot_nt(eye, row)[:, 0:1], (CHUNK, LANES)))
        seg_cols.append(jnp.broadcast_to(dot_nt(tri, row)[:, 0:1], (CHUNK, LANES)))
        seg_rows.append(dot_nt(row, tri)[0:1, :])
    keep = 1.0 - jnp.concatenate(ds_cols, axis=0)
    tok = lax.broadcasted_iota(jnp.int32, (n_tok, LANES), 0)
    m1 = keep
    k1 = jnp.where(tok >= 1, pltpu.roll(keep, 1, 0), 1.0)
    k2 = jnp.where(tok >= 2, pltpu.roll(keep, 2, 0), 1.0)
    mk[0] = m1
    mk[1] = m1 * k1
    mk[2] = m1 * k1 * k2

    xcopy.wait()
    wcopy(jnp.int32(1)).start()
    bcopy.start()
    hrow = lax.broadcasted_iota(jnp.int32, (HALO, LANES), 0)
    k_last = jnp.broadcast_to(mk[0, n_tok - 8:n_tok, :][7:8, :], (HALO, LANES))
    k_last2 = jnp.broadcast_to(mk[1, n_tok - 8:n_tok, :][7:8, :], (HALO, LANES))
    hmask = jnp.where(hrow == HALO - 1, 1.0, jnp.where(hrow == HALO - 2, k_last, jnp.where(hrow == HALO - 3, k_last2, 0.0)))
    for q in range(d_model // LANES):
        hal[:, q * LANES:(q + 1) * LANES] = (xe[n_tok:n_tok + HALO, q * LANES:(q + 1) * LANES].astype(F32) * hmask).astype(BF16)

    def zblock(t, zi):
        wnext(t)
        slot = lax.rem(t, 3)
        zb[zi] = dot_nt(xe[HALO:HALO + n_tok], wbuf[slot]).astype(BF16)

    pl.semaphore_wait(barrier, n_chip + 1)
    halo_send = pltpu.make_async_remote_copy(
        src_ref=hal, dst_ref=xe.at[pl.ds(0, HALO)], send_sem=hs_sem, recv_sem=hr_sem,
        device_id=dev(lax.rem(me + 1, n_seq)), device_id_type=MESH)

    @pl.when(me < n_seq - 1)
    def _():
        halo_send.start()

    @pl.when(me == 0)
    def _():
        xe[0:HALO, :] = jnp.zeros((HALO, d_model), BF16)

    @pl.loop(0, n_zfirst)
    def _(t):
        zblock(t, t)

    @pl.when(me > 0)
    def _():
        halo_send.wait_recv()

    bcopy.wait()
    lane = lax.broadcasted_iota(jnp.int32, (1, LANES), 1)
    p_bcd = dot_nt(xe[...], wbcd[...]).astype(BF16).astype(F32)
    for lt in range(2 * state_dim // LANES + 1):
        us2[lt] = p_bcd[:, lt * LANES:(lt + 1) * LANES]

    def udot(slot, u_ref):
        p_u = dot_nt(xe[...], wbuf[slot]).astype(BF16).astype(F32)
        for lt in range(n_lt):
            u_ref[lt] = p_u[:, lt * LANES:(lt + 1) * LANES]

    t_u = n_zfirst
    wnext(jnp.int32(t_u))
    udot(t_u % 3, us)

    def conv(u_ref, r0, lt, wl):
        wl = pl.multiple_of(wl, LANES)
        cw = cw_ref[:, pl.ds(wl, LANES)] * 0.5
        v = cb_ref[pl.ds(wl // LANES, 1), :] * 0.5 + cw[0:1] * u_ref[lt, pl.ds(r0 + HALO, ROWS), :]
        for k in range(1, 4):
            v = v + cw[k:k + 1] * (mk[k - 1, pl.ds(r0, ROWS), :] * u_ref[lt, pl.ds(r0 + HALO - k, ROWS), :])
        return half_silu(v)

    for r0 in range(0, n_tok, ROWS):
        for lt in range(2 * state_dim // LANES):
            bc[r0:r0 + ROWS, lt * LANES:(lt + 1) * LANES] = conv(us2, r0, lt, d_inner + lt * LANES).astype(BF16)

    prm[...] = jnp.zeros((8, LANES), F32)
    prm[0:1, 0:n_heads] = dtb_ref[...]
    prm[1:2, 0:n_heads] = alog_ref[...]
    prm[2:3, 0:n_heads] = dsk_ref[...]
    pv = prm[...]
    head_ok = lane < n_heads
    neg_a = jnp.where(head_ok, -jnp.exp(pv[1:2]) , 0.0)
    e_rows = []
    for c in range(n_chunks):
        rows = slice(c * CHUNK, (c + 1) * CHUNK)
        raw = jnp.where(head_ok, us2[2 * state_dim // LANES, HALO + c * CHUNK:HALO + (c + 1) * CHUNK, :], 0.0) + pv[0:1]
        dt = jnp.maximum(raw, 0.0) + jnp.log1p(jnp.exp(-jnp.abs(raw)))
        s1, s2, s3 = split3(neg_a * dt * LOG2E)
        acum = dot(tri, s3) + dot(tri, s2) + dot(tri, s1)
        a2[rows, :] = acum
        a_t = jnp.transpose(acum)
        ld_t = jnp.transpose(jnp.log2(dt))
        ldt[:, rows] = ld_t
        apt[:, rows] = a_t - ld_t
        seg = seg_cols[c]
        last = acum[CHUNK - 1:CHUNK, :]
        seg_last = seg[CHUNK - 1:CHUNK, :]
        ws[rows, :] = jnp.where(seg == 0.0, jnp.exp2(acum), 0.0)
        we[rows, :] = jnp.where(seg == seg_last, jnp.exp2(last - acum) * dt, 0.0)
        e_rows.append(jnp.where(seg_last == 0.0, jnp.exp2(last), 0.0))
        b_c = bc[rows, 0:state_dim]
        c_c = bc[rows, state_dim:2 * state_dim]
        b_t = jnp.transpose(b_c.astype(F32)).astype(BF16)
        bt[c] = b_t
        scores = dot(c_c, b_t)
        same = jnp.concatenate([seg] * per, axis=1) == seg_rows[c]
        gm[c] = jnp.where(jnp.logical_and(ri >= ci, same), scores, 0.0)
    d_own = e_rows[0] * e_rows[1]
    dec[0:1, :] = e_rows[0]
    dec[1:2, :] = e_rows[1]
    dpair[core] = jnp.broadcast_to(d_own, (8, LANES))

    pair_send = pltpu.make_async_remote_copy(
        src_ref=dpair.at[core], dst_ref=dpair.at[core], send_sem=dps_sem, recv_sem=dp_sem,
        device_id=dev(partner), device_id_type=MESH)
    pair_send.start()

    def send_decays():
        pair_send.wait()
        dchip[...] = dpair[0] * dpair[1]
        dg[chip] = dpair[0] * dpair[1]
        dec[2:3, :] = dpair[0][0:1]
        dec[3:4, :] = dpair[1][0:1]

        @pl.loop(1, n_chip)
        def _(r):
            q = lax.rem(chip + r, n_chip)
            pltpu.make_async_remote_copy(
                src_ref=dchip, dst_ref=dg.at[chip], send_sem=dgs_sem, recv_sem=dg_sem,
                device_id=dev(2 * q + core), device_id_type=MESH).start()

    def expand(v, b):
        n = v.shape[0]
        r = pltpu.roll(v, lax.rem(2 * LANES - hb * b, LANES), 1)
        low = lax.broadcasted_iota(jnp.int32, (n, LANES), 1) < head_dim
        out = []
        for p in range(n_lt):
            out.append(jnp.where(low, jnp.broadcast_to(r[:, 2 * p:2 * p + 1], (n, LANES)),
                                 jnp.broadcast_to(r[:, 2 * p + 1:2 * p + 2], (n, LANES))))
        return jnp.concatenate(out, axis=1)

    def roll_to(dst, src, b):
        sh = lax.rem(2 * LANES - hb * b, LANES)
        for q in range(n_tok // LANES):
            dst[q * LANES:(q + 1) * LANES, :] = pltpu.roll(src[q * LANES:(q + 1) * LANES, :], sh, 1)

    low_r = lax.broadcasted_iota(jnp.int32, (ROWS, LANES), 1) < head_dim

    def head_cols(r0, lt):
        wv = arl[pl.ds(r0, ROWS), :]
        return jnp.where(low_r, jnp.broadcast_to(wv[:, 2 * lt:2 * lt + 1], (ROWS, LANES)),
                         jnp.broadcast_to(wv[:, 2 * lt + 1:2 * lt + 2], (ROWS, LANES)))

    low_b = (lax.broadcasted_iota(jnp.int32, (CHUNK, LANES), 1) < head_dim).astype(F32).astype(BF16)
    high_b = (lax.broadcasted_iota(jnp.int32, (CHUNK, LANES), 1) >= head_dim).astype(F32).astype(BF16)

    sub = 32

    def intra(b):
        roll_to(arm, a2, b)
        heads = pl.ds(pl.multiple_of(b * hb, hb), hb)
        dsk = expand(prm[...], b)[2:3]
        for c in range(n_chunks):
            r0 = c * CHUNK
            ap8 = apt[heads, r0:r0 + CHUNK]
            ld8 = ldt[heads, r0:r0 + CHUNK]
            for p in range(n_lt):
                cols = slice(p * LANES, (p + 1) * LANES)
                k = p % 4
                for hh in range(2):
                    h = 2 * p + hh
                    aj0, aj1 = ap8[h:h + 1, :HALF], ap8[h:h + 1, HALF:]
                    ld0, ld1 = ld8[h:h + 1, :HALF], ld8[h:h + 1, HALF:]
                    base = CHUNK + hh * CHUNK
                    for q in range(HALF // sub):
                        rr = slice(q * sub, (q + 1) * sub)
                        g0 = slice(q * sub, (q + 1) * sub)
                        g1 = slice(HALF + q * sub, HALF + (q + 1) * sub)
                        ai0 = jnp.broadcast_to(arm[r0 + q * sub:r0 + (q + 1) * sub, h:h + 1], (sub, HALF))
                        ai1 = jnp.broadcast_to(arm[r0 + HALF + q * sub:r0 + HALF + (q + 1) * sub, h:h + 1], (sub, HALF))
                        mix[k, rr, hh * HALF:(hh + 1) * HALF] = (jnp.exp2(jnp.minimum(ai0 - aj0, ld0)) * gm[c, g0, 0:HALF]).astype(BF16)
                        mix[k, rr, base:base + HALF] = (jnp.exp2(ai1 - aj0) * gm[c, g1, 0:HALF]).astype(BF16)
                        mix[k, rr, base + HALF:base + CHUNK] = (jnp.exp2(jnp.minimum(ai1 - aj1, ld1)) * gm[c, g1, HALF:CHUNK]).astype(BF16)
                xp = xb[b, r0:r0 + CHUNK, cols]
                xa, xh = xp * low_b, xp * high_b
                y0 = dot(mix[k, :, 0:CHUNK], jnp.concatenate([xa[:HALF], xh[:HALF]], axis=0))
                y1 = dot(mix[k, :, CHUNK:3 * CHUNK], jnp.concatenate([xa, xh], axis=0))
                yb[b, r0:r0 + HALF, cols] = y0 + dsk[:, cols] * xp[:HALF].astype(F32)
                yb[b, r0 + HALF:r0 + CHUNK, cols] = y1 + dsk[:, cols] * xp[HALF:].astype(F32)

    def ublock(t_next, u_next, u_ref, b, t_ref, b_done):
        wnext(t_next)
        slot = lax.rem(t_next, 3)
        roll_to(arl, we, b)
        udot(slot, u_next)
        for r0 in range(0, n_tok, ROWS):
            for lt in range(n_lt):
                cols = slice(lt * LANES, (lt + 1) * LANES)
                xs = conv(u_ref, r0, lt, b * LB + lt * LANES).astype(BF16)
                xb[b, r0:r0 + ROWS, cols] = xs
                sc[r0:r0 + ROWS, cols] = (xs.astype(F32) * head_cols(r0, lt)).astype(BF16)

        intra(b_done)
        ex = expand(dec[...], b)
        st0 = dot(bt[0], sc[0:CHUNK])
        cs0[b] = st0
        t_ref[...] = ex[1:2] * st0 + dot(bt[1], sc[CHUNK:2 * CHUNK])

    def part_copy(i):
        return pltpu.make_async_remote_copy(
            src_ref=tsend.at[i], dst_ref=two.at[i, core], send_sem=ps_sem.at[i], recv_sem=pr_sem.at[i],
            device_id=dev(partner), device_id_type=MESH)

    def home_copy(i, q):
        return pltpu.make_async_remote_copy(
            src_ref=tc.at[i, q], dst_ref=hrecv.at[i, chip], send_sem=s1_sem.at[i], recv_sem=r1_sem.at[i],
            device_id=dev(2 * q + core), device_id_type=MESH)

    def back_copy(i, q):
        return pltpu.make_async_remote_copy(
            src_ref=hout.at[i, q], dst_ref=s0r.at[i, chip], send_sem=s2_sem.at[i], recv_sem=r2_sem.at[i],
            device_id=dev(2 * q + core), device_id_type=MESH)

    def all_copies(src, dst, send_sem, recv_sem):
        return pltpu.make_async_remote_copy(
            src_ref=src.at[pl.ds(0, n_chip - 1)], dst_ref=dst.at[pl.ds(0, n_chip - 1)], send_sem=send_sem, recv_sem=recv_sem,
            device_id=dev(partner), device_id_type=MESH)

    def fin_copy(i):
        return pltpu.make_async_remote_copy(
            src_ref=fbuf.at[i, 1 - core], dst_ref=soth.at[i], send_sem=fs_sem.at[i], recv_sem=fr_sem.at[i],
            device_id=dev(partner), device_id_type=MESH)

    def send_home(i, b):
        part_copy(i).wait_recv()
        ex = expand(dec[...], b)
        for q in range(n_chip):
            rows = slice(q * hrows, (q + 1) * hrows)
            tc[i, q] = ex[3:4] * two[i, 0, rows] + two[i, 1, rows]
        hrecv[i, chip] = tc[i, chip]

        @pl.loop(1, n_chip, unroll=True)
        def _(r):
            home_copy(i, lax.rem(chip + r, n_chip)).start()

    def home(i):
        b = 2 * i + core
        all_copies(tc.at[i], hrecv.at[i], s1_sem.at[i], r1_sem.at[i]).wait_recv()
        ex = expand(dga[...], b)
        run = jnp.zeros((hrows, LB), F32)
        for q in range(n_chip):
            hout[i, q] = run
            run = ex[q:q + 1] * run + hrecv[i, q]
        s0r[i, chip] = hout[i, chip]

        @pl.loop(1, n_chip, unroll=True)
        def _(r):
            back_copy(i, lax.rem(chip + r, n_chip)).start()

    def finish(i):
        b = 2 * i + core
        all_copies(hout.at[i], s0r.at[i], s2_sem.at[i], r2_sem.at[i]).wait_recv()
        ex = expand(dec[...], b)
        for q in range(n_chip):
            rows = slice(q * hrows, (q + 1) * hrows)
            fbuf[i, 0, rows] = s0r[i, q]
            fbuf[i, 1, rows] = ex[2:3] * s0r[i, q] + two[i, 0, rows]
        fin_copy(i).start()

    @pl.loop(0, npair)
    def _(i):
        t = n_zfirst + 2 * i
        ublock(t + 1, us2, us, 2 * i + 1 - core, tsend.at[i], 2 * jnp.maximum(i - 1, 0) + core)
        part_copy(i).start()

        @pl.when(i == 0)
        def _():
            send_decays()

        ublock(t + 2, us, us2, 2 * i + core, two.at[i, core], 2 * i + 1 - core)
        send_home(i, 2 * i + core)

        @pl.when(i == 0)
        def _():
            all_copies(dg, dg, dgs_sem, dg_sem).wait_recv()
            for q in range(n_chip):
                dga[q:q + 1, :] = dg[q, 0:1, :]

        @pl.when(i >= 1)
        def _():
            home(i - 1)

        @pl.when(i >= 3)
        def _():
            finish(i - 3)

    for lt in range(n_lt):
        zb[n_zfirst, :, lt * LANES:(lt + 1) * LANES] = us[lt, HALO:HALO + n_tok, :].astype(BF16)

    def zdot(t, zi):
        slot = lax.rem(t, 3)
        zb[zi] = dot_nt(xe[HALO:HALO + n_tok], wbuf[slot]).astype(BF16)

    @pl.loop(0, n_zmid)
    def _(m):
        t = t_z + 1 + m
        wnext(t)
        zdot(t, n_zfirst + 2 * (m + 1))

        @pl.when(m == 0)
        def _():
            finish(npair - 3)

        @pl.when(m == 1)
        def _():
            intra(2 * (npair - 1) + core)

        @pl.when(m == n_zmid - 1)
        def _():
            home(npair - 1)

    ssq[...] = jnp.zeros((n_tok, LANES), F32)

    def close(b, s_ref):
        ex = expand(dec[...], b)
        roll_to(arl, ws, b)
        s_in = s_ref[...]
        yst[0:CHUNK, :] = dot(bc[0:CHUNK, state_dim:2 * state_dim], s_in.astype(BF16))
        s_mid = ex[0:1] * s_in + cs0[b]
        yst[CHUNK:2 * CHUNK, :] = dot(bc[CHUNK:2 * CHUNK, state_dim:2 * state_dim], s_mid.astype(BF16))

        @pl.loop(0, n_tok // ROWS, unroll=True)
        def _(q):
            rows = pl.ds(pl.multiple_of(q * ROWS, ROWS), ROWS)
            acc = ssq[rows, :]
            for lt in range(n_lt):
                cols = slice(lt * LANES, (lt + 1) * LANES)
                y = yb[b, rows, cols] + head_cols(q * ROWS, lt) * yst[rows, cols]
                gated = y * half_silu(zb[b, rows, cols].astype(F32) * 0.5)
                yb[b, rows, cols] = gated
                acc = acc + gated * gated
            ssq[rows, :] = acc

    @pl.loop(0, npair)
    def _(i):
        fin_copy(i).wait_recv()
        t = t_z + n_zmid + 1 + i

        @pl.when(i < n_zlast)
        def _():
            wnext(t)

        zdot(jnp.minimum(t, 2 * nb - 1), jnp.where(i < n_zlast, n_zfirst + 1 + 2 * i, nb))
        close(2 * i + core, fbuf.at[i, core])
        close(2 * i + 1 - core, soth.at[i])

        @pl.when(i == 0)
        def _():
            finish(npair - 2)

        @pl.when(i == npair - 3)
        def _():
            finish(npair - 1)

    scale = lax.rsqrt(jnp.sum(ssq[...], axis=1, keepdims=True) * (1.0 / d_inner) + EPS)
    ssq[...] = jnp.broadcast_to(scale, (n_tok, LANES))

    n_out = d_model // LB

    def normalize(b):
        @pl.loop(0, n_tok // ROWS, unroll=True)
        def _(q):
            rows = pl.ds(pl.multiple_of(q * ROWS, ROWS), ROWS)
            sv = ssq[rows, :]
            for lt in range(n_lt):
                cols = slice(lt * LANES, (lt + 1) * LANES)
                nw = nw_ref[:, pl.ds(pl.multiple_of(b * LB + lt * LANES, LANES), LANES)]
                zb[b, rows, cols] = (yb[b, rows, cols] * sv * nw).astype(BF16)

    @pl.loop(0, n_out)
    def _(b):
        normalize(b)

    def ocopy(n):
        return pltpu.make_async_copy(xb.at[n], o_hbm.at[:, n * LB:(n + 1) * LB], gsem.at[n])

    def project(b, first, last):
        wnext(b + 2 * nb)
        slot = lax.rem(b + 2 * nb, 3)
        for n in range(n_out):
            part = dot(zb[b], wbuf[slot, :, n * LB:(n + 1) * LB])
            if not first:
                part = yb[n] + part
            if last:
                xb[n] = part.astype(BF16)
                ocopy(n).start()
            else:
                yb[n] = part

    project(jnp.int32(0), True, False)

    @pl.loop(1, nb - 1)
    def _(b):
        @pl.when(b >= n_out - 1)
        def _():
            normalize(b + 1)
        project(b, False, False)

    project(jnp.int32(nb - 1), False, True)

    @pl.when(me < n_seq - 1)
    def _():
        halo_send.wait_send()

    all_copies(dg, dg, dgs_sem, dg_sem).wait_send()

    @pl.loop(0, npair)
    def _(i):
        part_copy(i).wait_send()
        all_copies(tc.at[i], hrecv.at[i], s1_sem.at[i], r1_sem.at[i]).wait_send()
        all_copies(hout.at[i], s0r.at[i], s2_sem.at[i], r2_sem.at[i]).wait_send()
        fin_copy(i).wait_send()

    for n in range(n_out):
        ocopy(n).wait()


def mixer(n_seq, x, doc_start, w_in, conv_w, conv_b, dt_bias, a_log, d_skip, norm_w, w_out):
    n_tok, d_model = x.shape
    d_inner = norm_w.shape[0] * norm_w.shape[1]
    n_heads = a_log.shape[0]
    state_dim = (conv_w.shape[1] - d_inner) // 2
    nb = d_inner // LB
    npair = nb // 2
    n_chip = n_seq // 2
    hrows = state_dim // n_chip
    dims = (n_seq, n_tok, d_model, d_inner, n_heads, state_dim)
    vmem = pl.BlockSpec(memory_space=pltpu.VMEM)
    anyspace = pl.BlockSpec(memory_space=pl.ANY)
    dma = pltpu.SemaphoreType.DMA
    scratch = [
        pltpu.VMEM((n_tok + HALO, d_model), BF16),
        pltpu.VMEM((3, LB, d_model), BF16),
        pltpu.VMEM((2 * state_dim + LANES, d_model), BF16),
        pltpu.VMEM((nb + 1, n_tok, LB), BF16),
        pltpu.VMEM((nb, n_tok, LB), BF16),
        pltpu.VMEM((nb, n_tok, LB), F32),
        pltpu.VMEM((LB // LANES, n_tok + HALO, LANES), F32),
        pltpu.VMEM((LB // LANES, n_tok + HALO, LANES), F32),
        pltpu.VMEM((n_tok, LB), F32),
        pltpu.VMEM((n_tok, LB), BF16),
        pltpu.VMEM((4, HALF, 3 * CHUNK), BF16),
        pltpu.VMEM((nb, state_dim, LB), F32),
        pltpu.VMEM((npair, state_dim, LB), F32),
        pltpu.VMEM((npair, 2, state_dim, LB), F32),
        pltpu.VMEM((npair, n_chip, hrows, LB), F32),
        pltpu.VMEM((npair, n_chip, hrows, LB), F32),
        pltpu.VMEM((npair, n_chip, hrows, LB), F32),
        pltpu.VMEM((npair, n_chip, hrows, LB), F32),
        pltpu.VMEM((npair, 2, state_dim, LB), F32),
        pltpu.VMEM((npair, state_dim, LB), F32),
        pltpu.VMEM((n_tok, 2 * state_dim), BF16),
        pltpu.VMEM((n_tok // CHUNK, state_dim, CHUNK), BF16),
        pltpu.VMEM((n_tok // CHUNK, CHUNK, CHUNK), F32),
        pltpu.VMEM((n_tok, LANES), F32),
        pltpu.VMEM((LANES, n_tok), F32),
        pltpu.VMEM((LANES, n_tok), F32),
        pltpu.VMEM((n_tok, LANES), F32),
        pltpu.VMEM((n_tok, LANES), F32),
        pltpu.VMEM((n_tok, LANES), F32),
        pltpu.VMEM((n_tok, LANES), F32),
        pltpu.VMEM((8, LANES), F32),
        pltpu.VMEM((8, LANES), F32),
        pltpu.VMEM((2, 8, LANES), F32),
        pltpu.VMEM((8, LANES), F32),
        pltpu.VMEM((n_chip, 8, LANES), F32),
        pltpu.VMEM((n_chip, LANES), F32),
        pltpu.VMEM((3, n_tok, LANES), F32),
        pltpu.VMEM((n_tok, LANES), F32),
        pltpu.VMEM((HALO, d_model), BF16),
        dma(()), dma((3,)), dma(()), dma(()), dma(()), dma(()), dma(()), dma(()), dma(()),
        dma((npair,)), dma((npair,)), dma((npair,)), dma((npair,)), dma((npair,)), dma((npair,)), dma((npair,)), dma((npair,)),
        dma((d_model // LB,)),
    ]
    return pl.pallas_call(
        functools.partial(mixer_kernel, dims),
        out_shape=jax.ShapeDtypeStruct((n_tok, d_model), BF16),
        in_specs=[anyspace, vmem, anyspace, anyspace, vmem, vmem, vmem, vmem, vmem, vmem],
        out_specs=anyspace,
        scratch_shapes=scratch,
        compiler_params=pltpu.CompilerParams(collective_id=0, has_side_effects=True, vmem_limit_bytes=66 * 1000 * 1000),
        name='mixer',
    )(x, doc_start.reshape(n_tok // LANES, LANES), w_in.T, w_out, conv_w, conv_b.reshape(-1, LANES), dt_bias.reshape(1, -1),
      a_log.reshape(1, -1), d_skip.reshape(1, -1), norm_w.reshape(1, -1))


def solution(mesh):
    n_seq = mesh.shape['sp']
    row_spec = P(('dp', 'sp'), None)
    tok_spec = P(('dp', 'sp'))

    def layer_shard(x, doc_start, w_in, conv_w, conv_b, dt_bias, a_log, d_skip, norm_w, w_out):
        return mixer(n_seq, x, doc_start, w_in, conv_w, conv_b, dt_bias, a_log, d_skip, norm_w, w_out)

    return jax.shard_map(layer_shard, mesh=mesh, in_specs=(row_spec, tok_spec, P(), P(), P(), P(), P(), P(), P(), P()), out_specs=row_spec, check_vma=False)
```
